256 devices in a mesh: dp: 32 (over z_lo, x, y), mp: 8 (over z_hi, core).
Axes of the slice: x: 4, y: 4, z: 8 (z_hi: 4, z_lo: 2; z = z_hi * 2 + z_lo), core: 2. Of those that a mesh axis runs over, the one named last changes fastest.
Arguments:
- hidden_states: bfloat16 [16384, 4096], P('dp', 'mp'), may hold values from -40 to 40
- norm_gain: float32 [1, 4096], replicated, may hold values from 0.1 to 1.9
- query_weight: bfloat16 [1, 4096, 4096], P(None, 'dp', 'mp'), may hold values from -0.01171875 to 0.01171875
- keyvalue_weight: bfloat16 [1, 4096, 2, 4096], P(None, 'dp', None, 'mp'), may hold values from -0.09375 to 0.09375
- output_weight: bfloat16 [1, 4096, 4096], P(None, 'dp', 'mp'), may hold values from -0.09375 to 0.09375
- position_bias: float32 [1, 32, 64], P(None, None, 'mp'), may hold values from -8 to 250
- lengths: int32 [128], P('dp'), may hold values from 16 to 128
Outputs:
- layer_output: bfloat16 [16384, 4096], P('dp', 'mp')
The draws below stay inside these ranges and needn't reach their ends.
All inputs are finite; a program needn't handle non-finite values.
Results may differ from the reference program's by a relative error of at most 0.006.
Values may be sent and summed in bfloat16 or wider, within the bound.
A program may use at most 128 MiB of HBM per device.

```python
import jax
import jax.numpy as jnp
import numpy as np
from jax import lax

D = 4096
HEADS = 64
DH = 64
BUCKETS = 32
DIST = 128
LEN = 128
LAYERS = 1
INNER = 4096
CAPTIONS = 128
TOKENS = 16384


def draw_hidden_states(key, part):
    key_rows, key_columns, key_noise = jax.random.split(key, 3)
    row_scale = jnp.exp(jax.random.uniform(key_rows, (TOKENS, 1), jnp.float32, np.log(0.3), np.log(3.0)))
    column_scale = jnp.exp(jax.random.uniform(key_columns, (1, D), jnp.float32, np.log(0.3), np.log(3.0)))
    gaussian = jax.random.normal(key_noise, (TOKENS, D), jnp.float32)
    values = row_scale * column_scale * gaussian
    return jnp.clip(values, -40.0, 40.0).astype(jnp.bfloat16)


def draw_position_bias(key, part):
    key_base = jax.random.fold_in(key, 0)
    baseline = jnp.clip(1.5 * jax.random.normal(key_base, (LAYERS, BUCKETS, HEADS), jnp.float32), -8.0, 8.0)
    return baseline


def set_ends(drawn, stream_key, low, top_value):
    longest = drawn.shape.index(max(drawn.shape))
    spots = []
    for shift in (0, 1):
        where = [jax.random.randint(jax.random.fold_in(stream_key, axis), (), 0, length) for axis, length in enumerate(drawn.shape)]
        where[longest] = (where[longest] + shift) % drawn.shape[longest]
        spots.append(tuple(where))
    return drawn.at[spots[0]].set(low).at[spots[1]].set(top_value)


def shard_levels(own_key, shape, cuts, smallest, top_value):
    def one(position, parts):
        steps = jax.random.uniform(jax.random.fold_in(jax.random.fold_in(own_key, 6), position), (parts,), jnp.float32, smallest / len(cuts), top_value / len(cuts))
        return jnp.repeat(jnp.exp(steps), shape[position] // parts).reshape((-1,) + (1,) * (len(shape) - position - 1))

    loudness = one(*cuts[0])
    for cut in cuts[1:]:
        loudness = loudness * one(*cut)
    return loudness


def centred(stream_key, extent, spread, limit, cuts=(), kind=jnp.bfloat16):
    drawn = jax.random.normal(stream_key, extent, jnp.float32) * spread
    if len(cuts) > 0:
        drawn = shard_levels(stream_key, extent, cuts, -0.22, 0.18) * drawn
    return jnp.clip(drawn, min=-limit, max=limit).astype(kind)


def setup_inputs(seed: int = 0) -> dict:
    arg_keys = jax.random.split(jax.random.key(seed), 8)
    return {
        "hidden_states": draw_hidden_states(jax.random.fold_in(arg_keys[7], 71), 0),
        "norm_gain": jnp.clip(1.0 + 0.18 * jax.random.normal(arg_keys[1], (LAYERS, D), jnp.float32), 0.1, 1.9),
        "query_weight": centred(arg_keys[2], (LAYERS, D, INNER), (D * DH) ** -0.5, 0.01171875, ((1, 32), (2, 8))),
        "keyvalue_weight": centred(arg_keys[3], (LAYERS, D, 2, INNER), D ** -0.5, 0.09375, ((1, 32), (3, 8))),
        "output_weight": centred(arg_keys[4], (LAYERS, D, INNER), INNER ** -0.5, 0.09375, ((1, 32), (2, 8))),
        "position_bias": draw_position_bias(jax.random.fold_in(arg_keys[7], 71), 0),
        "lengths": set_ends(jax.random.randint(arg_keys[6], (CAPTIONS,), LEN // 8, LEN + 1), jax.random.fold_in(arg_keys[6], 1), LEN // 8, LEN).astype(jnp.int32),
    }


epsilon = 1e-06

def bucket_table():
    half_count = BUCKETS // 2
    exact_count = half_count // 2
    positions = np.arange(LEN)
    relative = positions[None, :] - positions[:, None]
    distance = np.abs(relative)
    scaled = np.log(np.maximum(distance, 1) / exact_count) / np.log(DIST / exact_count) * (half_count - exact_count)
    far_bucket = np.minimum(exact_count + np.floor(scaled + 1e-09).astype(np.int32), half_count - 1)
    near_bucket = np.where(distance < exact_count, distance, far_bucket)
    return (near_bucket + np.where(relative > 0, half_count, 0)).astype(np.int32)

def normed_rows(hidden, gain_row):
    values = hidden.astype(jnp.float32)
    mean_square = lax.optimization_barrier(jnp.mean(values * values, axis=-1, keepdims=True))
    return (values * lax.rsqrt(mean_square + epsilon) * gain_row).astype(jnp.bfloat16)

def reference(hidden_states, norm_gain, query_weight, keyvalue_weight, output_weight, position_bias, lengths):
    buckets = bucket_table()
    hidden = hidden_states
    for layer_index in range(LAYERS):
        normed = normed_rows(hidden, norm_gain[layer_index])
        queries = jnp.dot(normed, query_weight[layer_index], preferred_element_type=jnp.float32).astype(jnp.bfloat16)
        paired = jnp.dot(normed, keyvalue_weight[layer_index].reshape(D, 2 * INNER), preferred_element_type=jnp.float32).astype(jnp.bfloat16)
        key_rows = paired[:, :INNER].reshape(CAPTIONS, LEN, HEADS, DH)
        value_rows = paired[:, INNER:].reshape(CAPTIONS, LEN, HEADS, DH)
        position_terms = jnp.transpose(position_bias[layer_index][buckets], (2, 0, 1))

        def attend_caption(inputs):
            query_block, key_block, value_block, length = inputs
            scores = jnp.einsum('qhe,khe->hqk', query_block.astype(jnp.float32), key_block.astype(jnp.float32)) + position_terms
            visible = jnp.arange(LEN) < length
            scores = jnp.where(visible[None, None, :], scores, -1e+30)
            maxima = lax.optimization_barrier(jnp.max(scores, axis=-1, keepdims=True))
            raised = jnp.exp(scores - maxima)
            weights = (raised / lax.optimization_barrier(jnp.sum(raised, axis=-1, keepdims=True))).astype(jnp.bfloat16)
            mixture = jnp.einsum('hqk,khe->qhe', weights.astype(jnp.float32), value_block.astype(jnp.float32))
            return mixture.astype(jnp.bfloat16).reshape(LEN, INNER)
        attended = lax.map(attend_caption, (queries.reshape(CAPTIONS, LEN, HEADS, DH), key_rows, value_rows, lengths))
        attended = attended.reshape(TOKENS, INNER)
        projected = jnp.dot(attended, output_weight[layer_index].T, preferred_element_type=jnp.float32)
        hidden = (hidden.astype(jnp.float32) + projected).astype(jnp.bfloat16)
    return hidden
```

```python
import functools

import jax
import jax.numpy as jnp
import numpy as np
from jax import lax
from jax.experimental import pallas as pl
from jax.experimental.pallas import tpu as pltpu
from jax.sharding import PartitionSpec as P

MESH = pl.DeviceIdType.MESH
DH = 64
BUCKETS = 32
DIST = 128
LEN = 128
EPS = 1e-06
F32 = jnp.float32
BF16 = jnp.bfloat16
NT = (((1,), (1,)), ((), ()))


def far_steps():
    half = BUCKETS // 2
    exact = half // 2
    distance = np.arange(LEN)
    scaled = np.log(np.maximum(distance, 1) / exact) / np.log(DIST / exact) * (half - exact)
    far = np.minimum(exact + np.floor(scaled + 1e-09).astype(np.int32), half - 1)
    near = np.where(distance < exact, distance, far)
    return [int(np.min(distance[near >= b])) for b in range(1, half) if np.any(near >= b)]


STEPS = far_steps()


def kernel(x_ref, g_ref, w_ref, pb_ref, mk_ref, o_ref,
           wb, hb, nb, qkv, att, ob, sb, rb, bt, pbs, mks, fs, fr,
           loc_sem, send_sem, hr, hd, wzs, wf, ws, wd, rr, sm, fin):
    dp = lax.axis_index("dp")
    mp = lax.axis_index("mp")
    zl, xi, yi = dp // 16, (dp // 4) % 4, dp % 4
    zh, c = mp // 2, mp % 2
    z = zh * 2 + zl
    oc = 1 - c
    oz = 1 - zl

    def dev(zz, xx, yy, cc):
        return ((zz % 2) * 16 + xx * 4 + yy, (zz // 2) * 2 + cc)

    xr, xl = (xi + 1) % 4, (xi + 3) % 4
    yr, yl = (yi + 1) % 4, (yi + 3) % 4
    zr, zf = (z + 1) % 8, (z + 7) % 8
    d_xr, d_xl = dev(z, xr, yi, c), dev(z, xl, yi, c)
    d_yr, d_yl = dev(z, xi, yr, c), dev(z, xi, yl, c)
    d_zr, d_zl = dev(zr, xi, yi, c), dev(zf, xi, yi, c)
    d_pc = dev(z, xi, yi, oc)
    d_zp = dev(zh * 2 + oz, xi, yi, c)

    pending = []

    def send(src, dst, sem, to, group):
        d = pltpu.make_async_remote_copy(
            src_ref=src, dst_ref=dst, send_sem=send_sem.at[group], recv_sem=sem,
            device_id=to, device_id_type=MESH)
        d.start()
        pending.append(d)

    def recv(dst, sem):
        pltpu.make_async_remote_copy(
            src_ref=dst, dst_ref=dst, send_sem=send_sem.at[0], recv_sem=sem,
            device_id=d_pc, device_id_type=MESH).wait_recv()

    barrier = pltpu.get_barrier_semaphore()
    for to in (d_xr, d_xl, d_yr, d_yl, d_zr, d_zl, d_pc):
        pl.semaphore_signal(barrier, inc=1, device_id=to, device_id_type=MESH)
    pl.semaphore_wait(barrier, 7)

    def blk(k, cls, f, s, h=None):
        zz = zl if cls == 0 else oz
        bx, by = (f, s) if cls == 0 else (s, f)
        if h is None:
            return wb.at[pl.ds(2 * k, 2), c, zz, bx, by]
        return wb.at[2 * k + h, c, zz, bx, by]

    def axes(cls):
        if cls == 0:
            return xi, xr, xl, d_xr, d_xl, yi, yr, yl, d_yr, d_yl
        return yi, yr, yl, d_yr, d_yl, xi, xr, xl, d_xr, d_xl

    def fo(cls, o):
        f = axes(cls)[0]
        return (f + (0, 3, 1, 2)[o]) % 4

    def S0(cls, k, src):
        f, fR, fL, dfR, dfL, s, sR, sL, dsR, dsL = axes(cls)
        own = blk(k, cls, f, s)
        send(src, own, wf.at[cls, k, 0], dfR, 0)
        send(src, own, wf.at[cls, k, 1], dfL, 0)
        send(src, own, ws.at[cls, k, 0, 0], dsR, 0)
        send(src, own, ws.at[cls, k, 0, 1], dsL, 0)

    def S1(cls, k):
        f, fR, fL, dfR, dfL, s, sR, sL, dsR, dsL = axes(cls)
        recv(blk(k, cls, fL, s), wf.at[cls, k, 0])
        recv(blk(k, cls, fR, s), wf.at[cls, k, 1])
        send(blk(k, cls, fL, s, 0), blk(k, cls, fL, s, 0), wf.at[cls, k, 2], dfR, 0)
        send(blk(k, cls, fR, s, 1), blk(k, cls, fR, s, 1), wf.at[cls, k, 3], dfL, 0)
        for o, ff in ((1, fL), (2, fR)):
            b = blk(k, cls, ff, s)
            send(b, b, ws.at[cls, k, o, 0], dsR, 0)
            send(b, b, ws.at[cls, k, o, 1], dsL, 0)

    def S2(cls, k):
        f, fR, fL, dfR, dfL, s, sR, sL, dsR, dsL = axes(cls)
        ff = (f + 2) % 4
        recv(blk(k, cls, ff, s, 0), wf.at[cls, k, 2])
        recv(blk(k, cls, ff, s, 1), wf.at[cls, k, 3])
        b = blk(k, cls, ff, s)
        send(b, b, ws.at[cls, k, 3, 0], dsR, 0)
        send(b, b, ws.at[cls, k, 3, 1], dsL, 0)

    def Y(cls, k, o):
        f, fR, fL, dfR, dfL, s, sR, sL, dsR, dsL = axes(cls)
        ff = fo(cls, o)
        recv(blk(k, cls, ff, sL), ws.at[cls, k, o, 0])
        recv(blk(k, cls, ff, sR), ws.at[cls, k, o, 1])
        send(blk(k, cls, ff, sL, 0), blk(k, cls, ff, sL, 0), ws.at[cls, k, o, 2], dsR, 0)
        send(blk(k, cls, ff, sR, 1), blk(k, cls, ff, sR, 1), ws.at[cls, k, o, 3], dsL, 0)

    def dslice(k, cls, ff, cc):
        if cls == 0:
            return wb.at[pl.ds(2 * k, 2), cc, zl, ff]
        return wb.at[pl.ds(2 * k, 2), cc, oz, :, ff]

    def Z(cls, k, o):
        f, fR, fL, dfR, dfL, s, sR, sL, dsR, dsL = axes(cls)
        ff = fo(cls, o)
        s2 = (s + 2) % 4
        recv(blk(k, cls, ff, s2, 0), ws.at[cls, k, o, 2])
        recv(blk(k, cls, ff, s2, 1), ws.at[cls, k, o, 3])
        piece = dslice(k, cls, ff, c)
        send(piece, piece, wd.at[cls, k, o], d_pc, 0)

    def hpiece(zo, hh, j):
        return hb.at[(zo // 2) * 2 + hh, pl.ds(((zo % 2) * 2 + j) * LEN, LEN)]

    def hsend(right, r, hh):
        zo = (z - r + 8) % 8 if right else (z + r) % 8
        for j in range(2):
            p = hpiece(zo, hh, j)
            send(p, p, hr.at[0 if right else 1, r, hh, j], d_zr if right else d_zl, 0)

    def hrecv(right, r, hh):
        zo = (z - 1 - r + 8) % 8 if right else (z + 1 + r) % 8
        for j in range(2):
            recv(hpiece(zo, hh, j), hr.at[0 if right else 1, r, hh, j])

    def hstep(r, hh):
        for right in (True, False):
            full = r < 3 or (hh == 0) == right
            if not full:
                continue
            hrecv(right, r, hh)
            if r + 1 < 3 or (r + 1 == 3 and (hh == 0) == right):
                hsend(right, r + 1, hh)

    w_own = [w_ref.at[zl, pl.ds(2 * k, 2)] for k in range(2)]
    w_far = [w_ref.at[oz, pl.ds(2 * k, 2)] for k in range(2)]
    for j in range(2):
        send(x_ref.at[pl.ds((oc * 2 + j) * LEN, LEN)],
             hb.at[mp, pl.ds((zl * 2 + j) * LEN, LEN)], hd.at[j], d_pc, 0)
    for k in range(2):
        send(w_far[k], wb.at[pl.ds(2 * k, 2), c, zl, xi, yi], wzs.at[k], d_zp, 0)
    for k in range(2):
        S0(0, k, w_own[k])
    send(pb_ref.at[pl.ds(zl * 4, 4)], pbs.at[c], sm.at[0], d_pc, 0)
    send(mk_ref, mks.at[zl], sm.at[1], d_zp, 0)
    locs = []
    for j in range(2):
        locs.append(pltpu.make_async_copy(
            x_ref.at[pl.ds((c * 2 + j) * LEN, LEN)],
            hb.at[mp, pl.ds((zl * 2 + j) * LEN, LEN)], loc_sem.at[j]))
    for k in range(2):
        locs.append(pltpu.make_async_copy(w_own[k], blk(k, 0, xi, yi), loc_sem.at[2 + k]))
    locs.append(pltpu.make_async_copy(pb_ref.at[pl.ds(zl * 4, 4)], pbs.at[c], loc_sem.at[4]))
    locs.append(pltpu.make_async_copy(mk_ref, mks.at[zl], loc_sem.at[5]))
    for d in locs:
        d.start()
    for d in locs:
        d.wait()
    for j in range(2):
        recv(hb.at[zh * 2 + oc, pl.ds((zl * 2 + j) * LEN, LEN)], hd.at[j])
    for hh in range(2):
        hsend(True, 0, hh)
        hsend(False, 0, 1 - hh)

    def zx(k):
        b = blk(k, 1, yi, xi)
        recv(b, wzs.at[k])
        S0(1, k, b)

    S1(0, 0)
    zx(0)
    S1(0, 1)
    zx(1)
    hstep(0, 0)
    Y(0, 0, 0)
    Y(0, 1, 0)
    hstep(0, 1)
    S1(1, 0)
    Y(1, 0, 0)
    S1(1, 1)
    Y(1, 1, 0)
    S2(0, 0)
    S2(0, 1)
    hstep(1, 0)
    S2(1, 0)
    S2(1, 1)
    for cls in range(2):
        Y(cls, 0, 1)
        Y(cls, 0, 2)
    hstep(1, 1)
    for cls in range(2):
        Y(cls, 1, 1)
        Y(cls, 1, 2)
        Z(cls, 0, 0)
        Z(cls, 1, 0)

    recv(pbs.at[oc], sm.at[0])
    recv(mks.at[oz], sm.at[1])
    row = lax.broadcasted_iota(jnp.int32, (LEN, LEN), 0)
    col = lax.broadcasted_iota(jnp.int32, (LEN, LEN), 1)
    rel = col - row
    dist = jnp.abs(rel)
    bucket = jnp.where(rel > 0, BUCKETS // 2, 0)
    for t in STEPS:
        bucket = bucket + jnp.where(dist >= t, 1, 0)

    def bias_head(i, _):
        cc, h = i // 4, i % 4
        tab = jnp.zeros((LEN, LEN), F32)
        for b in range(BUCKETS):
            tab = jnp.where(bucket == b, pbs[cc, h, pl.ds(b, 1), :], tab)
        bt[cc, pl.ds(pl.multiple_of(h * LEN, LEN), LEN), :] = tab
        return 0

    lax.fori_loop(0, 8, bias_head, 0)

    hstep(2, 0)
    for cls in range(2):
        Y(cls, 0, 3)
    for cls in range(2):
        Y(cls, 1, 3)
    hstep(2, 1)
    for o in (1, 2):
        for cls in range(2):
            Z(cls, 0, o)
            Z(cls, 1, o)
    hstep(3, 0)
    hstep(3, 1)
    for cls in range(2):
        Z(cls, 0, 3)
        Z(cls, 1, 3)

    def norm_rows(i, _):
        rows = pl.ds(pl.multiple_of(i * 16, 16), 16)
        total = jnp.zeros((16, 512), F32)
        for fb in range(8):
            v = hb[fb, rows, :].astype(F32)
            total = total + v * v
        ms = jnp.sum(total, axis=-1, keepdims=True) * (1.0 / 4096.0)
        scale = lax.rsqrt(ms + EPS)
        for fb in range(8):
            v = hb[fb, rows, :].astype(F32)
            nb[rows, fb * 512:(fb + 1) * 512] = (
                v * scale * g_ref[:, fb * 512:(fb + 1) * 512]).astype(BF16)
        return 0

    lax.fori_loop(0, 32, norm_rows, 0)

    for o in range(4):
        for cls in range(2):
            for k in range(2):
                ff = fo(cls, o)
                recv(dslice(k, cls, ff, oc), wd.at[cls, k, o])

    def project(i, _):
        m, cc = i // 2, i % 2
        w = wb[m, cc].reshape(4096, 256)
        qkv[m, cc] = jnp.dot(nb[...], w, preferred_element_type=F32).astype(BF16)
        return 0

    lax.fori_loop(0, 6, project, 0)

    head = lax.broadcasted_iota(jnp.int32, (LEN, 256), 1) // DH

    def attend(i, _):
        cap, cc = i // 2, i % 2
        rows = pl.ds(pl.multiple_of(cap * LEN, LEN), LEN)
        q, kk, v = qkv[0, cc, rows, :], qkv[1, cc, rows, :], qkv[2, cc, rows, :]
        zero = jnp.zeros((), BF16)
        qm = jnp.concatenate([jnp.where(head == h, q, zero) for h in range(4)], axis=0)
        s = lax.dot_general(qm, kk, NT, preferred_element_type=F32) + bt[cc]
        seen = mks[cap // 2, pl.ds(2 * c + cap % 2, 1), :]
        s = jnp.where(seen > 0.5, s, -1e30)
        top = jnp.max(s, axis=-1, keepdims=True)
        e = jnp.exp(s - top)
        w = (e / jnp.sum(e, axis=-1, keepdims=True)).astype(BF16)
        mix = jnp.dot(w, v, preferred_element_type=F32)
        out = jnp.zeros((LEN, 256), F32)
        for h in range(4):
            out = jnp.where(head == h, mix[h * LEN:(h + 1) * LEN], out)
        att[cc, rows, :] = out.astype(BF16)
        return 0

    lax.fori_loop(0, 8, attend, 0)

    def out_block(zq):
        for hh in range(2):
            total = None
            for cc in range(2):
                w = wb[3, cc, hh_zl(zq, hh), hh_x(zq, hh)].reshape(512, 256)
                part = lax.dot_general(att[cc], w, NT, preferred_element_type=F32)
                total = part if total is None else total + part
            ob[zq * 2 + hh] = total

    def hh_zl(zq, hh):
        return (zq * 2 + hh) // 4

    def hh_x(zq, hh):
        return (zq * 2 + hh) % 4

    def own(dz, hh, j):
        return ob[(dz // 2) * 2 + hh, pl.ds(((dz % 2) * 2 + j) * LEN, LEN), :]

    def rs_round(r):
        for j in range(2):
            for hh in range(2):
                for right in (True, False):
                    side = 0 if right else 1
                    first = (hh == 0) == right
                    dz = (z + 4 - r) % 8 if right else (z + 4 + r) % 8
                    if r == 0 and not first:
                        continue
                    value = own(dz, hh, j)
                    if r >= 2 or (r == 1 and first):
                        recv(rb.at[side, r - 1, hh, j], rr.at[side, r - 1, hh, j])
                        value = value + rb[side, r - 1, hh, j].astype(F32)
                    sb[side, r, hh, j] = value.astype(BF16)
                    send(sb.at[side, r, hh, j], rb.at[side, r, hh, j],
                         rr.at[side, r, hh, j], d_zr if right else d_zl, 0)

    out_block((zh + 2) % 4)
    rs_round(0)
    out_block((zh + 1) % 4)
    out_block((zh + 3) % 4)
    rs_round(1)
    out_block(zh)
    rs_round(2)
    rs_round(3)

    def finish(hh, j):
        for side in range(2):
            recv(rb.at[side, 3, hh, j], rr.at[side, 3, hh, j])
        rows = pl.ds((zl * 2 + j) * LEN, LEN)
        return (hb[zh * 2 + hh, rows, :].astype(F32) + own(z, hh, j)
                + rb[0, 3, hh, j].astype(F32) + rb[1, 3, hh, j].astype(F32)).astype(BF16)

    for j in range(2):
        fs[j] = finish(oc, j)
        send(fs.at[j], fr.at[j], fin.at[j], d_pc, 0)
        o_ref[pl.ds((c * 2 + j) * LEN, LEN), :] = finish(c, j)
    for j in range(2):
        recv(fr.at[j], fin.at[j])
        o_ref[pl.ds((oc * 2 + j) * LEN, LEN), :] = fr[j]

    for d in pending:
        d.wait_send()


def local(hidden_states, norm_gain, query_weight, keyvalue_weight, output_weight,
          position_bias, lengths):
    kv = jnp.transpose(keyvalue_weight[0], (1, 0, 2))
    w = jnp.stack([query_weight[0], kv[0], kv[1], output_weight[0]])
    w = jnp.transpose(w.reshape(4, 128, 2, 256), (2, 0, 1, 3))
    pb = jnp.broadcast_to(jnp.transpose(position_bias[0])[:, :, None], (8, BUCKETS, LEN))
    mask = (jnp.arange(LEN)[None, :] < lengths[:, None]).astype(F32)
    mask = jnp.concatenate([mask, jnp.zeros((4, LEN), F32)])
    vm = pl.BlockSpec(memory_space=pltpu.VMEM)
    dma = pltpu.SemaphoreType.DMA
    return pl.pallas_call(
        kernel,
        out_shape=jax.ShapeDtypeStruct((512, 512), BF16),
        in_specs=[vm] * 5,
        out_specs=vm,
        scratch_shapes=[
            pltpu.VMEM((4, 2, 2, 4, 4, 128, 256), BF16),
            pltpu.VMEM((8, 512, 512), BF16),
            pltpu.VMEM((512, 4096), BF16),
            pltpu.VMEM((3, 2, 512, 256), BF16),
            pltpu.VMEM((2, 512, 256), BF16),
            pltpu.VMEM((8, 512, 512), F32),
            pltpu.VMEM((2, 4, 2, 2, 128, 512), BF16),
            pltpu.VMEM((2, 4, 2, 2, 128, 512), BF16),
            pltpu.VMEM((2, 512, 128), F32),
            pltpu.VMEM((2, 4, BUCKETS, LEN), F32),
            pltpu.VMEM((2, 8, LEN), F32),
            pltpu.VMEM((2, 128, 512), BF16),
            pltpu.VMEM((2, 128, 512), BF16),
            dma((6,)),
            dma((1,)),
            dma((2, 4, 2, 2)),
            dma((2,)),
            dma((2,)),
            dma((2, 2, 4)),
            dma((2, 2, 4, 4)),
            dma((2, 2, 4)),
            dma((2, 4, 2, 2)),
            dma((2,)),
            dma((2,)),
        ],
        compiler_params=pltpu.CompilerParams(
            collective_id=0, has_side_effects=True, vmem_limit_bytes=60 * 1024 * 1024),
        name="t5_attention",
    )(hidden_states, norm_gain, w, pb, mask)


def solution(mesh):
    in_specs = (
        P("dp", "mp"),
        P(),
        P(None, "dp", "mp"),
        P(None, "dp", None, "mp"),
        P(None, "dp", "mp"),
        P(None, None, "mp"),
        P("dp"),
    )
    return jax.shard_map(local, mesh=mesh, in_specs=in_specs, out_specs=P("dp", "mp"), check_vma=False)
```

```python
import functools

import jax
import jax.numpy as jnp
import numpy as np
from jax import lax
from jax.experimental import pallas as pl
from jax.experimental.pallas import tpu as pltpu
from jax.sharding import PartitionSpec as P

MESH = pl.DeviceIdType.MESH
DH = 64
BUCKETS = 32
DIST = 128
LEN = 128
EPS = 1e-06
F32 = jnp.float32
BF16 = jnp.bfloat16
NT = (((1,), (1,)), ((), ()))


def far_steps():
    half = BUCKETS // 2
    exact = half // 2
    distance = np.arange(LEN)
    scaled = np.log(np.maximum(distance, 1) / exact) / np.log(DIST / exact) * (half - exact)
    far = np.minimum(exact + np.floor(scaled + 1e-09).astype(np.int32), half - 1)
    near = np.where(distance < exact, distance, far)
    return [int(np.min(distance[near >= b])) for b in range(1, half) if np.any(near >= b)]


STEPS = far_steps()


LINKS = ("x+", "x-", "y+", "y-", "z+", "z-", "d")
RATE = {"d": 400e3}
COST = {"norm": 1.0, "proj": 0.9, "attn": 0.55, "out": 0.5, "bias": 2.2, "rs": 0.25, "fin": 0.4}
AHEAD = 3.0


def flip(d):
    return "-" if d == "+" else "+"


def make_tasks():
    tasks = {}

    def add(tid, link, kib, needs, rank):
        tasks[tid] = (link, kib, tuple(needs), rank)

    for j in range(2):
        add(("HD", j), "d", 128, (), 0)
    for m in range(4):
        add(("ZX", m), "z", 64, (), 0.5 if m < 3 else 14)
    for j in range(2):
        for d in "+-":
            for r in range(4):
                for hh in range(2):
                    if r == 3 and (hh == 0) != (d == "+"):
                        continue
                    need = [("HD", j)] if r == 0 and hh == 1 else []
                    if r > 0:
                        need = [("H", d, r - 1, hh, j)]
                    add(("H", d, r, hh, j), "z" + d, 128, need, 1 + 20 * j + r)
    for m in range(4):
        late = 10 if m == 3 else 0
        for cls in range(2):
            fa, sa = ("x", "y") if cls == 0 else ("y", "x")
            base = [("ZX", m)] if cls else []
            for d in "+-":
                add(("F", cls, m, d), fa + d, 64, base, m + late)
                add(("S", cls, m, 0, d), sa + d, 64, base, m + late + 1)
                add(("S", cls, m, 1, d), sa + d, 64, [("F", cls, m, "+")], m + late + 1)
                add(("S", cls, m, 2, d), sa + d, 64, [("F", cls, m, "-")], m + late + 1)
                add(("S", cls, m, 3, d), sa + d, 64, [("F2", cls, m)], m + late)
            d = "+-"[(m + cls) % 2]
            add(("F2", cls, m), fa + d, 64, [("F", cls, m, d)], m + late - 1)
            for o in range(4):
                d = "+-"[(m + cls + o) % 2]
                add(("S2", cls, m, o), sa + d, 64, [("S", cls, m, o, d)], m + late + 0.5)
                add(("D", cls, m, o), "d", 256,
                    [("S", cls, m, o, "+"), ("S", cls, m, o, "-"), ("S2", cls, m, o)], m + late)

    def mine(m):
        return ([("ZX", m)] + [("F", c, m, d) for c in range(2) for d in "+-"]
                + [("F2", c, m) for c in range(2)]
                + [("S", c, m, o, d) for c in range(2) for o in range(4) for d in "+-"]
                + [("S2", c, m, o) for c in range(2) for o in range(4)])

    def theirs(m):
        return [("D", c, m, o) for c in range(2) for o in range(4)]

    add(("bias",), None, 0, (), 60)
    for j in range(2):
        add(("norm", j), None, 0,
            [("HD", j)] + [t for t in tasks if t[0] == "H" and t[4] == j], 40 + j)
        for m in range(3):
            add(("proj", m, 0, j), None, 0, [("norm", j)] + mine(m), 42 + 20 * j + 2 * m)
            add(("proj", m, 1, j), None, 0, [("norm", j)] + theirs(m), 43 + 20 * j + 2 * m)
        for cc in range(2):
            for q in range(2):
                add(("attn", q, cc, j), None, 0,
                    [("bias",)] + [("proj", m, cc, j) for m in range(3)], 48 + 20 * j)
        for n, step in enumerate((2, 1, 3, 0)):
            add(("out", step, j), None, 0,
                [("attn", q, cc, j) for q in range(2) for cc in range(2)] + mine(3) + theirs(3),
                50 + 20 * j + n)
        for d in "+-":
            for r in range(4):
                for hh in range(2):
                    first = (hh == 0) == (d == "+")
                    if r == 0 and not first:
                        continue
                    steps = {0: (2,), 1: (2, 1, 3), 2: (1, 3, 2), 3: (0, 1, 2, 3)}[r]
                    need = [("out", step, j) for step in steps]
                    if r >= 2 or (r == 1 and first):
                        need.append(("R", d, r - 1, hh, j))
                    add(("R", d, r, hh, j), "z" + d, 128, need, 30 + 20 * j - r)
        for hh in (1, 0):
            add(("fin", hh, j), "d" if hh else None, 128,
                [("out", 0, j), ("R", "+", 3, hh, j), ("R", "-", 3, hh, j)], 30 + j)
    return tasks


def list_schedule():
    tasks = make_tasks()
    free = dict.fromkeys(LINKS, 0.0)
    arrive, finished, order = {}, {}, []
    left = dict(tasks)
    now = 0.0

    def ready_at(tid):
        t = 0.0
        for n in tasks[tid][2]:
            when = arrive.get(n) if tasks[n][0] else finished.get(n)
            if when is None:
                return None
            t = max(t, when)
        return t

    while left:
        best, soonest = None, None
        for tid in left:
            link, kib, _, rank = tasks[tid]
            at = ready_at(tid)
            if at is None:
                continue
            links = ("z+", "z-") if link == "z" else (link,) if link else ()
            for one in links:
                at = max(at, free[one] - AHEAD)
            if at <= now + 1e-9:
                key = (0 if link else 1, rank, str(tid))
                if best is None or key < best[0]:
                    best = (key, tid, links)
            elif soonest is None or at < soonest:
                soonest = at
        if best is None:
            now = soonest
            continue
        _, tid, links = best
        link, kib, _, _ = tasks[tid]
        kind = {"R": "rs"}.get(tid[0], tid[0])
        now += COST.get(kind, 0.06)
        finished[tid] = now
        if link:
            rate = RATE.get(link, 46.6e3) / 1.024e3
            t = max([now] + [free[one] for one in links]) + kib / rate
            for one in links:
                free[one] = t
            arrive[tid] = t + (1.0 if link == "d" else 1.8)
        order.append(tid)
        del left[tid]
    return tasks, order, finished, arrive


def kernel(x_ref, g_ref, w_ref, pb_ref, mk_ref, o_ref,
           wb, hb, nb, qkv, att, ob, sb, rb, bt, pbs, mks, fs, fr,
           loc_sem, send_sem, hr, hd, wzs, wf, wf2, ws, ws2, wd, rr, sm, fin):
    dp = lax.axis_index("dp")
    mp = lax.axis_index("mp")
    zl, xi, yi = dp // 16, (dp // 4) % 4, dp % 4
    zh, c = mp // 2, mp % 2
    z = zh * 2 + zl
    oc = 1 - c
    oz = 1 - zl

    def dev(zz, xx, yy, cc):
        return ((zz % 2) * 16 + xx * 4 + yy, (zz // 2) * 2 + cc)

    xp, xm = (xi + 1) % 4, (xi + 3) % 4
    yp, ym = (yi + 1) % 4, (yi + 3) % 4
    devices = {
        "x+": dev(z, xp, yi, c), "x-": dev(z, xm, yi, c),
        "y+": dev(z, xi, yp, c), "y-": dev(z, xi, ym, c),
        "z+": dev((z + 1) % 8, xi, yi, c), "z-": dev((z + 7) % 8, xi, yi, c),
        "d": dev(z, xi, yi, oc), "z": dev(zh * 2 + oz, xi, yi, c),
    }
    pending = []

    def send(src, dst, sem, link):
        d = pltpu.make_async_remote_copy(
            src_ref=src, dst_ref=dst, send_sem=send_sem.at[0], recv_sem=sem,
            device_id=devices[link], device_id_type=MESH)
        d.start()
        pending.append(d)

    def recv(dst, sem):
        pltpu.make_async_remote_copy(
            src_ref=dst, dst_ref=dst, send_sem=send_sem.at[0], recv_sem=sem,
            device_id=devices["d"], device_id_type=MESH).wait_recv()

    barrier = pltpu.get_barrier_semaphore()
    for link in LINKS:
        pl.semaphore_signal(barrier, inc=1, device_id=devices[link], device_id_type=MESH)
    pl.semaphore_wait(barrier, len(LINKS))

    def blk(m, cls, f, s):
        bx, by = (f, s) if cls == 0 else (s, f)
        return wb.at[m, c, zl if cls == 0 else oz, bx, by]

    def axes(cls):
        return ("x", "y", xi, yi) if cls == 0 else ("y", "x", yi, xi)

    def step(i, d):
        return (i + (1 if d == "+" else 3)) % 4

    def fblock(cls, o):
        f = axes(cls)[2]
        return (f + (0, 3, 1, 2)[o]) % 4

    def dslice(m, cls, ff, cc):
        if cls == 0:
            return wb.at[m, cc, zl, ff]
        return wb.at[m, cc, oz, :, ff]

    def col(zz, hh):
        return (zz // 2) * 2 + (c if hh == 0 else oc)

    def rows(zz, j):
        return pl.ds(pl.multiple_of((j * 2 + zz % 2) * LEN, LEN), LEN)

    def hpiece(zo, hh, j):
        return hb.at[col(zo, hh), rows(zo, j)]

    def side(d):
        return 0 if d == "+" else 1

    def issue(t):
        kind = t[0]
        if kind == "HD":
            send(x_ref.at[pl.ds((oc * 2 + t[1]) * LEN, LEN)], hb.at[mp, rows(z, t[1])], hd.at[t[1]], "d")
        elif kind == "ZX":
            send(w_ref.at[oz, t[1]], wb.at[t[1], c, zl, xi, yi], wzs.at[t[1]], "z")
        elif kind == "H":
            _, d, r, hh, j = t
            zo = (z + 8 - r) % 8 if d == "+" else (z + r) % 8
            p = hpiece(zo, hh, j)
            send(p, p, hr.at[side(d), r, hh, j], "z" + d)
        elif kind == "F":
            _, cls, m, d = t
            fa, sa, f, s = axes(cls)
            own = blk(m, cls, f, s)
            send(w_ref.at[zl, m] if cls == 0 else own, own, wf.at[cls, m, side(d)], fa + d)
        elif kind == "F2":
            _, cls, m = t
            fa, sa, f, s = axes(cls)
            d = "+-"[(m + cls) % 2]
            b = blk(m, cls, step(f, flip(d)), s)
            send(b, b, wf2.at[cls, m], fa + d)
        elif kind == "S":
            _, cls, m, o, d = t
            fa, sa, f, s = axes(cls)
            b = blk(m, cls, fblock(cls, o), s)
            send(w_ref.at[zl, m] if cls == 0 and o == 0 else b, b, ws.at[cls, m, o, side(d)], sa + d)
        elif kind == "S2":
            _, cls, m, o = t
            fa, sa, f, s = axes(cls)
            d = "+-"[(m + cls + o) % 2]
            b = blk(m, cls, fblock(cls, o), step(s, flip(d)))
            send(b, b, ws2.at[cls, m, o], sa + d)
        elif kind == "D":
            _, cls, m, o = t
            p = dslice(m, cls, fblock(cls, o), c)
            send(p, p, wd.at[cls, m, o], "d")
        elif kind == "R":
            _, d, r, hh, j = t
            first = (hh == 0) == (d == "+")
            dz = (z + 4 - r) % 8 if d == "+" else (z + 4 + r) % 8
            value = ob[col(dz, hh), rows(dz, j), :]
            if r >= 2 or (r == 1 and first):
                value = value + rb[side(d), r - 1, hh, j].astype(F32)
            sb[side(d), r, hh, j] = value.astype(BF16)
            send(sb.at[side(d), r, hh, j], rb.at[side(d), r, hh, j], rr.at[side(d), r, hh, j], "z" + d)
        elif kind == "fin":
            _, hh, j = t
            value = (hb[col(z, hh), rows(z, j), :].astype(F32) + ob[col(z, hh), rows(z, j), :]
                     + rb[0, 3, hh, j].astype(F32) + rb[1, 3, hh, j].astype(F32)).astype(BF16)
            if hh:
                fs[j] = value
                send(fs.at[j], fr.at[j], fin.at[j], "d")
            else:
                o_ref[pl.ds((c * 2 + j) * LEN, LEN), :] = value
        elif kind == "bias":
            bias()
        elif kind == "norm":
            norm(t[1])
        elif kind == "proj":
            _, m, cc, j = t
            who = c if cc == 0 else oc
            w = wb[m, who].reshape(4096, 256)
            half = slice(j * 256, j * 256 + 256)
            qkv[m, who, half, :] = jnp.dot(
                nb[half, :], w, preferred_element_type=F32).astype(BF16)
        elif kind == "attn":
            attend(*t[1:])
        elif kind == "out":
            zq = (zh + t[1]) % 4
            half = slice(t[2] * 256, t[2] * 256 + 256)
            for hh in range(2):
                fb = zq * 2 + hh
                total = None
                for cc in range(2):
                    w = wb[3, cc, fb // 4, fb % 4].reshape(512, 256)
                    part = lax.dot_general(att[cc, half, :], w, NT, preferred_element_type=F32)
                    total = part if total is None else total + part
                ob[fb, half, :] = total

    def land(t):
        kind = t[0]
        if kind == "HD":
            recv(hb.at[zh * 2 + oc, rows(z, t[1])], hd.at[t[1]])
        elif kind == "ZX":
            recv(blk(t[1], 1, yi, xi), wzs.at[t[1]])
        elif kind == "H":
            _, d, r, hh, j = t
            zo = (z + 7 - r) % 8 if d == "+" else (z + 1 + r) % 8
            recv(hpiece(zo, hh, j), hr.at[side(d), r, hh, j])
        elif kind == "F":
            _, cls, m, d = t
            fa, sa, f, s = axes(cls)
            recv(blk(m, cls, step(f, flip(d)), s), wf.at[cls, m, side(d)])
        elif kind == "F2":
            _, cls, m = t
            fa, sa, f, s = axes(cls)
            recv(blk(m, cls, (f + 2) % 4, s), wf2.at[cls, m])
        elif kind == "S":
            _, cls, m, o, d = t
            fa, sa, f, s = axes(cls)
            recv(blk(m, cls, fblock(cls, o), step(s, flip(d))), ws.at[cls, m, o, side(d)])
        elif kind == "S2":
            _, cls, m, o = t
            fa, sa, f, s = axes(cls)
            recv(blk(m, cls, fblock(cls, o), (s + 2) % 4), ws2.at[cls, m, o])
        elif kind == "D":
            _, cls, m, o = t
            recv(dslice(m, cls, fblock(cls, o), oc), wd.at[cls, m, o])
        elif kind == "R":
            _, d, r, hh, j = t
            recv(rb.at[side(d), r, hh, j], rr.at[side(d), r, hh, j])

    def bias():
        recv(pbs.at[oc], sm.at[0])
        recv(mks.at[oz], sm.at[1])
        row = lax.broadcasted_iota(jnp.int32, (LEN, LEN), 0)
        lane = lax.broadcasted_iota(jnp.int32, (LEN, LEN), 1)
        rel = lane - row
        dist = jnp.abs(rel)
        bucket = jnp.where(rel > 0, BUCKETS // 2, 0)
        for t in STEPS:
            bucket = bucket + jnp.where(dist >= t, 1, 0)

        def bias_head(i, _):
            cc, h = i // 4, i % 4
            tab = jnp.zeros((LEN, LEN), F32)
            for b in range(BUCKETS):
                tab = jnp.where(bucket == b, pbs[cc, h, pl.ds(b, 1), :], tab)
            bt[cc, pl.ds(pl.multiple_of(h * LEN, LEN), LEN), :] = tab
            return 0

        lax.fori_loop(0, 8, bias_head, 0)

    def norm(j):
        def norm_rows(i, _):
            at = pl.ds(pl.multiple_of(i * 16, 16), 16)
            total = jnp.zeros((16, 512), F32)
            for fb in range(8):
                v = hb[fb, at, :].astype(F32)
                total = total + v * v
            ms = jnp.sum(total, axis=-1, keepdims=True) * (1.0 / 4096.0)
            scale = lax.rsqrt(ms + EPS)
            for fb in range(8):
                v = hb[fb, at, :].astype(F32)
                nb[at, fb * 512:(fb + 1) * 512] = (
                    v * scale * g_ref[:, fb * 512:(fb + 1) * 512]).astype(BF16)
            return 0

        lax.fori_loop(j * 16, j * 16 + 16, norm_rows, 0)

    def attend(q, cc, j):
        head = lax.broadcasted_iota(jnp.int32, (LEN, 256), 1) // DH
        who = c if cc == 0 else oc
        at = slice((j * 2 + q) * LEN, (j * 2 + q + 1) * LEN)
        qq, kk, v = qkv[0, who, at, :], qkv[1, who, at, :], qkv[2, who, at, :]
        zero = jnp.zeros((), BF16)
        qm = jnp.concatenate([jnp.where(head == h, qq, zero) for h in range(4)], axis=0)
        s = lax.dot_general(qm, kk, NT, preferred_element_type=F32) + bt[who]
        seen = mks[q, pl.ds(2 * c + j, 1), :]
        s = jnp.where(seen > 0.5, s, -1e30)
        top = jnp.max(s, axis=-1, keepdims=True)
        e = jnp.exp(s - top)
        w = (e / jnp.sum(e, axis=-1, keepdims=True)).astype(BF16)
        mix = jnp.dot(w, v, preferred_element_type=F32)
        out = jnp.zeros((LEN, 256), F32)
        for h in range(4):
            out = jnp.where(head == h, mix[h * LEN:(h + 1) * LEN], out)
        att[who, at, :] = out.astype(BF16)

    locs = []
    for j in range(2):
        locs.append(pltpu.make_async_copy(
            x_ref.at[pl.ds((c * 2 + j) * LEN, LEN)], hb.at[mp, rows(z, j)], loc_sem.at[j]))
    for m in range(4):
        locs.append(pltpu.make_async_copy(w_ref.at[zl, m], blk(m, 0, xi, yi), loc_sem.at[2 + m]))
    locs.append(pltpu.make_async_copy(pb_ref.at[pl.ds(zl * 4, 4)], pbs.at[c], loc_sem.at[6]))
    locs.append(pltpu.make_async_copy(mk_ref, mks.at[zl], loc_sem.at[7]))
    for d in locs:
        d.start()
    send(pb_ref.at[pl.ds(zl * 4, 4)], pbs.at[c], sm.at[0], "d")
    send(mk_ref, mks.at[zl], sm.at[1], "z")
    for d in locs:
        d.wait()

    tasks, order, _, _ = list_schedule()
    landed = set()
    for t in order:
        for n in tasks[t][2]:
            if tasks[n][0] and n not in landed:
                land(n)
                landed.add(n)
        issue(t)
    for t in order:
        if tasks[t][0] and t[0] != "fin" and t not in landed:
            land(t)
    for j in range(2):
        recv(fr.at[j], fin.at[j])
        o_ref[pl.ds((oc * 2 + j) * LEN, LEN), :] = fr[j]
    for d in pending:
        d.wait_send()


def local(hidden_states, norm_gain, query_weight, keyvalue_weight, output_weight,
          position_bias, lengths):
    kv = jnp.transpose(keyvalue_weight[0], (1, 0, 2))
    w = jnp.stack([query_weight[0], kv[0], kv[1], output_weight[0]])
    w = jnp.transpose(w.reshape(4, 128, 2, 256), (2, 0, 1, 3))
    pb = jnp.broadcast_to(jnp.transpose(position_bias[0])[:, :, None], (8, BUCKETS, LEN))
    mask = (jnp.arange(LEN)[None, :] < lengths[:, None]).astype(F32)
    mask = jnp.concatenate([mask, jnp.zeros((4, LEN), F32)])
    vm = pl.BlockSpec(memory_space=pltpu.VMEM)
    dma = pltpu.SemaphoreType.DMA
    return pl.pallas_call(
        kernel,
        out_shape=jax.ShapeDtypeStruct((512, 512), BF16),
        in_specs=[vm] * 5,
        out_specs=vm,
        scratch_shapes=[
            pltpu.VMEM((4, 2, 2, 4, 4, 128, 256), BF16),
            pltpu.VMEM((8, 512, 512), BF16),
            pltpu.VMEM((512, 4096), BF16),
            pltpu.VMEM((3, 2, 512, 256), BF16),
            pltpu.VMEM((2, 512, 256), BF16),
            pltpu.VMEM((8, 512, 512), F32),
            pltpu.VMEM((2, 4, 2, 2, 128, 512), BF16),
            pltpu.VMEM((2, 4, 2, 2, 128, 512), BF16),
            pltpu.VMEM((2, 512, 128), F32),
            pltpu.VMEM((2, 4, BUCKETS, LEN), F32),
            pltpu.VMEM((2, 8, LEN), F32),
            pltpu.VMEM((2, 128, 512), BF16),
            pltpu.VMEM((2, 128, 512), BF16),
            dma((8,)),
            dma((1,)),
            dma((2, 4, 2, 2)),
            dma((2,)),
            dma((4,)),
            dma((2, 4, 2)),
            dma((2, 4)),
            dma((2, 4, 4, 2)),
            dma((2, 4, 4)),
            dma((2, 4, 4)),
            dma((2, 4, 2, 2)),
            dma((2,)),
            dma((2,)),
        ],
        compiler_params=pltpu.CompilerParams(
            collective_id=0, has_side_effects=True, vmem_limit_bytes=60 * 1024 * 1024),
        name="t5_attention",
    )(hidden_states, norm_gain, w, pb, mask)


def solution(mesh):
    in_specs = (
        P("dp", "mp"),
        P(),
        P(None, "dp", "mp"),
        P(None, "dp", None, "mp"),
        P(None, "dp", "mp"),
        P(None, None, "mp"),
        P("dp"),
    )
    return jax.shard_map(local, mesh=mesh, in_specs=in_specs, out_specs=P("dp", "mp"), check_vma=False)
```

```python
import functools

import jax
import jax.numpy as jnp
import numpy as np
from jax import lax
from jax.experimental import pallas as pl
from jax.experimental.pallas import tpu as pltpu
from jax.sharding import PartitionSpec as P

MESH = pl.DeviceIdType.MESH
DH = 64
BUCKETS = 32
DIST = 128
LEN = 128
EPS = 1e-06
F32 = jnp.float32
BF16 = jnp.bfloat16
NT = (((1,), (1,)), ((), ()))


def far_steps():
    half = BUCKETS // 2
    exact = half // 2
    distance = np.arange(LEN)
    scaled = np.log(np.maximum(distance, 1) / exact) / np.log(DIST / exact) * (half - exact)
    far = np.minimum(exact + np.floor(scaled + 1e-09).astype(np.int32), half - 1)
    near = np.where(distance < exact, distance, far)
    return [int(np.min(distance[near >= b])) for b in range(1, half) if np.any(near >= b)]


STEPS = far_steps()


LINKS = ("x+", "x-", "y+", "y-", "zp", "zn", "d")
RATE = {"d": 400e3}
COST = {"norm": 1.2, "proj": 0.65, "attn": 0.35, "out": 0.4, "bias": 1.6, "rs": 0.2, "fin": 0.3,
        "prep": 1.0, "small": 0.4}
AHEAD = 3.0


H_HOPS = {(0, 0): 4, (1, 0): 3, (0, 1): 4, (1, 1): 3}
R_HOPS = {(0, 0): 4, (1, 0): 3, (0, 1): 4, (1, 1): 3}


def flip(d):
    return {"+": "-", "-": "+", "p": "n", "n": "p"}[d]


def rounds(hops, d, r):
    side = d if r % 2 == 0 else flip(d)
    return hops if side == "p" else 7 - hops


OUT_NEED = {("p", 0): ("own",), ("p", 1): ("p",), ("p", 2): ("p",), ("p", 3): ("far",),
            ("n", 0): ("n",), ("n", 1): ("n",), ("n", 2): ("far",), ("n", 3): ("far",)}
RANK = {"zx": (-14.4, 33.6, 2.8, 33.7), "h": (18.2, 34.9), "w": (4.1, 4.4, -0.5, 13.9), "f": -6.4, "s0": -19.3, "s1": 0.0,
        "s3": 9.7, "f2": -21.4, "s2": -5.3, "r": 58.5}


def make_tasks():
    tasks = {}

    def add(tid, link, kib, needs, rank):
        tasks[tid] = (link, kib, tuple(needs), rank)

    add(("prep",), None, 0, (), 0.2)
    add(("small",), None, 0, [("prep",)], 30)
    for j in range(2):
        add(("HD", j), "d", 128, (), 0)
    for m in range(4):
        add(("ZX", m), "zp", 64, [("prep",)] if m in (1, 2) else (), RANK["zx"][m])
    for j in range(2):
        for d in "pn":
            for r in range(4):
                for hh in range(2):
                    if r >= rounds(H_HOPS[hh, j], d, r):
                        continue
                    need = [("HD", j)] if r == 0 and hh == 1 else []
                    if r > 0:
                        need = [("H", flip(d), r - 1, hh, j)]
                    add(("H", d, r, hh, j), "z" + d, 128, need, RANK["h"][j] + r)
    for m in range(4):
        late = RANK["w"][m]
        for cls in range(2):
            fa, sa = ("x", "y") if cls == 0 else ("y", "x")
            base = [("ZX", m)] if cls else [("prep",)] if m in (1, 2) else []
            for d in "+-":
                add(("F", cls, m, d), fa + d, 64, base, late + RANK["f"])
                add(("S", cls, m, 0, d), sa + d, 64, base, late + RANK["s0"])
                add(("S", cls, m, 1, d), sa + d, 64, [("F", cls, m, "+")], late + RANK["s1"])
                add(("S", cls, m, 2, d), sa + d, 64, [("F", cls, m, "-")], late + RANK["s1"])
                add(("S", cls, m, 3, d), sa + d, 64, [("F2", cls, m)], late + RANK["s3"])
            d = "+-"[(m + cls) % 2]
            add(("F2", cls, m), fa + d, 64, [("F", cls, m, d)], late + RANK["f2"])
            for o in range(4):
                d = "+-"[(m + cls + o) % 2]
                add(("S2", cls, m, o), sa + d, 64, [("S", cls, m, o, d)], late + RANK["s2"])
                add(("D", cls, m, o), "d", 256,
                    [("S", cls, m, o, "+"), ("S", cls, m, o, "-"), ("S2", cls, m, o)]
                    + ([("small",)] if o == 0 else []), late)

    def mine(m):
        return ([("ZX", m)] + [("F", c, m, d) for c in range(2) for d in "+-"]
                + [("F2", c, m) for c in range(2)]
                + [("S", c, m, o, d) for c in range(2) for o in range(4) for d in "+-"]
                + [("S2", c, m, o) for c in range(2) for o in range(4)])

    def theirs(m):
        return [("D", c, m, o) for c in range(2) for o in range(4)]

    add(("bias",), None, 0, [("small",)], 60)
    for j in range(2):
        add(("norm", j), None, 0,
            [("HD", j)] + [t for t in tasks if t[0] == "H" and t[4] == j], 40 + j)
        for m in range(3):
            add(("proj", m, 0, j), None, 0, [("norm", j), ("small",)] + mine(m), 42 + 20 * j + 2 * m)
            add(("proj", m, 1, j), None, 0, [("norm", j)] + theirs(m), 43 + 20 * j + 2 * m)
        for cc in range(2):
            for q in range(2):
                add(("attn", q, cc, j), None, 0,
                    [("bias",)] + [("proj", m, cc, j) for m in range(3)], 48 + 20 * j)
        for n, step in enumerate(("far", "n", "p", "own")):
            add(("out", step, j), None, 0,
                [("attn", q, cc, j) for q in range(2) for cc in range(2)] + mine(3) + theirs(3),
                50 + 20 * j + n)
        for d in "pn":
            for r in range(4):
                for hh in range(2):
                    hops = rounds(R_HOPS[hh, j], d, r)
                    if r >= hops:
                        continue
                    need = [("out", step, j) for step in (OUT_NEED[d, r])]
                    if r < hops - 1:
                        need.append(("R", flip(d), r + 1, hh, j))
                    add(("R", d, r, hh, j), "z" + d, 128, need, 33 + RANK["r"] * j - r)
        for hh in (1, 0):
            add(("fin", hh, j), "d" if hh else None, 128,
                [("out", "own", j), ("R", "p", 0, hh, j), ("R", "n", 0, hh, j)], 30 + j)
    return tasks


def list_schedule():
    tasks = make_tasks()
    free = dict.fromkeys(LINKS, 0.0)
    arrive, finished, order = {}, {}, []
    left = dict(tasks)
    now = 0.0

    def ready_at(tid):
        t = 0.0
        for n in tasks[tid][2]:
            when = arrive.get(n) if tasks[n][0] else finished.get(n)
            if when is None:
                return None
            t = max(t, when)
        return t

    while left:
        best, soonest = None, None
        for tid in left:
            link, kib, _, rank = tasks[tid]
            at = ready_at(tid)
            if at is None:
                continue
            links = (link,) if link else ()
            for one in links:
                at = max(at, free[one] - AHEAD)
            if at <= now + 1e-9:
                key = (0 if link else 1, rank, str(tid))
                if best is None or key < best[0]:
                    best = (key, tid, links)
            elif soonest is None or at < soonest:
                soonest = at
        if best is None:
            now = soonest
            continue
        _, tid, links = best
        link, kib, _, _ = tasks[tid]
        kind = {"R": "rs"}.get(tid[0], tid[0])
        now += COST.get(kind, 0.06)
        finished[tid] = now
        if link:
            rate = RATE.get(link, 44.0e3) / 1.024e3
            t = max([now] + [free[one] for one in links]) + kib / rate
            for one in links:
                free[one] = t
            arrive[tid] = t + (1.0 if link == "d" else 1.8)
        order.append(tid)
        del left[tid]
    return tasks, order, finished, arrive


def kernel(x_ref, g_hbm, q_hbm, kv_hbm, ow_hbm, pb_hbm, len_hbm, o_ref,
           wb, hb, nb, qkv, att, ob, sb, rb, bt, pbs, mks, fs, fr,
           wq, wo, wkv, kvs, g_ref, pbv, lens,
           loc_sem, send_sem, hr, hd, wzs, wf, wf2, ws, ws2, wd, rr, sm, fin):
    dp = lax.axis_index("dp")
    mp = lax.axis_index("mp")
    zl, xi, yi = dp // 16, (dp // 4) % 4, dp % 4
    zh, c = mp // 2, mp % 2
    z = zh * 2 + zl
    oc = 1 - c
    oz = 1 - zl

    toward = 1 - 2 * zl

    def zstep(d, n):
        return (z + 8 + (toward if d == "p" else -toward) * n) % 8

    def dev(zz, xx, yy, cc):
        return ((zz % 2) * 16 + xx * 4 + yy, (zz // 2) * 2 + cc)

    xp, xm = (xi + 1) % 4, (xi + 3) % 4
    yp, ym = (yi + 1) % 4, (yi + 3) % 4
    devices = {
        "x+": dev(z, xp, yi, c), "x-": dev(z, xm, yi, c),
        "y+": dev(z, xi, yp, c), "y-": dev(z, xi, ym, c),
        "zp": dev(zstep("p", 1), xi, yi, c), "zn": dev(zstep("n", 1), xi, yi, c),
        "d": dev(z, xi, yi, oc),
    }
    pending = []

    def send(src, dst, sem, link):
        d = pltpu.make_async_remote_copy(
            src_ref=src, dst_ref=dst, send_sem=send_sem.at[0], recv_sem=sem,
            device_id=devices[link], device_id_type=MESH)
        d.start()
        pending.append(d)

    def recv(dst, sem):
        pltpu.make_async_remote_copy(
            src_ref=dst, dst_ref=dst, send_sem=send_sem.at[0], recv_sem=sem,
            device_id=devices["d"], device_id_type=MESH).wait_recv()

    lanes = pl.ds(pl.multiple_of(zl * 256, 256), 256)
    far_lanes = pl.ds(pl.multiple_of(oz * 256, 256), 256)

    def source(m, at):
        if m == 0:
            return wq.at[:, at]
        if m == 3:
            return wo.at[:, at]
        return kvs.at[m - 1, :, at]

    def col(zz, hh):
        return (zz // 2) * 2 + (c if hh == 0 else oc)

    def rows(zz, j):
        return pl.ds(pl.multiple_of((j * 2 + zz % 2) * LEN, LEN), LEN)

    def local(i, src, dst):
        d = pltpu.make_async_copy(src, dst, loc_sem.at[i])
        d.start()
        return d

    own_x = [local(j, x_ref.at[pl.ds((c * 2 + j) * LEN, LEN)], hb.at[mp, rows(z, j)]) for j in range(2)]
    own_q = local(2, q_hbm, wq)
    own_kv = local(3, kv_hbm, wkv)
    own_o = local(4, ow_hbm, wo)
    rest = [local(5, pb_hbm, pbv), local(6, len_hbm, lens), local(7, g_hbm, g_ref),
            local(8, q_hbm.at[:, lanes], wb.at[0, c, zl, xi, yi]),
            local(9, ow_hbm.at[:, lanes], wb.at[3, c, zl, xi, yi])]

    barrier = pltpu.get_barrier_semaphore()
    for link in LINKS:
        pl.semaphore_signal(barrier, inc=1, device_id=devices[link], device_id_type=MESH)
    pl.semaphore_wait(barrier, len(LINKS))

    def blk(m, cls, f, s):
        bx, by = (f, s) if cls == 0 else (s, f)
        return wb.at[m, c, zl if cls == 0 else oz, bx, by]

    def axes(cls):
        return ("x", "y", xi, yi) if cls == 0 else ("y", "x", yi, xi)

    def step(i, d):
        return (i + (1 if d == "+" else 3)) % 4

    def fblock(cls, o):
        f = axes(cls)[2]
        return (f + (0, 3, 1, 2)[o]) % 4

    def dslice(m, cls, ff, cc):
        if cls == 0:
            return wb.at[m, cc, zl, ff]
        return wb.at[m, cc, oz, :, ff]

    def hpiece(zo, hh, j):
        return hb.at[col(zo, hh), rows(zo, j)]

    def side(d):
        return 0 if d in "+p" else 1

    waits = {"x0": own_x[0], "x1": own_x[1], "q": own_q, "o": own_o}

    def gate(t):
        key = None
        if t[0] == "H" and t[2] == 0 and t[3] == 0:
            key = "x%d" % t[4]
        elif t[0] in ("ZX", "F", "S"):
            m = t[1] if t[0] == "ZX" else t[2]
            key = {0: "q", 3: "o"}.get(m)
        if key in waits:
            waits.pop(key).wait()

    def issue(t):
        kind = t[0]
        if kind == "HD":
            send(x_ref.at[pl.ds((oc * 2 + t[1]) * LEN, LEN)], hb.at[mp, rows(z, t[1])], hd.at[t[1]], "d")
        elif kind == "ZX":
            send(source(t[1], far_lanes), wb.at[t[1], c, zl, xi, yi], wzs.at[t[1]], "zp")
        elif kind == "H":
            _, d, r, hh, j = t
            p = hpiece(zstep(flip(d), r), hh, j)
            send(p, p, hr.at[side(d), r, hh, j], "z" + d)
        elif kind == "F":
            _, cls, m, d = t
            fa, sa, f, s = axes(cls)
            own = blk(m, cls, f, s)
            send(source(m, lanes) if cls == 0 else own, own, wf.at[cls, m, side(d)], fa + d)
        elif kind == "F2":
            _, cls, m = t
            fa, sa, f, s = axes(cls)
            d = "+-"[(m + cls) % 2]
            b = blk(m, cls, step(f, flip(d)), s)
            send(b, b, wf2.at[cls, m], fa + d)
        elif kind == "S":
            _, cls, m, o, d = t
            fa, sa, f, s = axes(cls)
            b = blk(m, cls, fblock(cls, o), s)
            send(source(m, lanes) if cls == 0 and o == 0 else b, b, ws.at[cls, m, o, side(d)], sa + d)
        elif kind == "S2":
            _, cls, m, o = t
            fa, sa, f, s = axes(cls)
            d = "+-"[(m + cls + o) % 2]
            b = blk(m, cls, fblock(cls, o), step(s, flip(d)))
            send(b, b, ws2.at[cls, m, o], sa + d)
        elif kind == "D":
            _, cls, m, o = t
            p = dslice(m, cls, fblock(cls, o), c)
            send(p, p, wd.at[cls, m, o], "d")
        elif kind == "R":
            _, d, r, hh, j = t
            dz = zstep(d, r + 1)
            value = ob[col(dz, hh), rows(dz, j), :]
            if r < rounds(R_HOPS[hh, j], d, r) - 1:
                value = value + rb[side(flip(d)), r + 1, hh, j].astype(F32)
            sb[side(d), r, hh, j] = value.astype(BF16)
            send(sb.at[side(d), r, hh, j], rb.at[side(d), r, hh, j], rr.at[side(d), r, hh, j], "z" + d)
        elif kind == "fin":
            _, hh, j = t
            value = (hb[col(z, hh), rows(z, j), :].astype(F32) + ob[col(z, hh), rows(z, j), :]
                     + rb[0, 0, hh, j].astype(F32) + rb[1, 0, hh, j].astype(F32)).astype(BF16)
            if hh:
                fs[j] = value
                send(fs.at[j], fr.at[j], fin.at[j], "d")
            else:
                o_ref[pl.ds((c * 2 + j) * LEN, LEN), :] = value
        elif kind == "prep":
            prep()
        elif kind == "small":
            small()
        elif kind == "bias":
            bias()
        elif kind == "norm":
            norm(t[1])
        elif kind == "proj":
            _, m, cc, j = t
            who = c if cc == 0 else oc
            w = wb[m, who].reshape(4096, 256)
            half = slice(j * 256, j * 256 + 256)
            qkv[m, who, half, :] = jnp.dot(
                nb[half, :], w, preferred_element_type=F32).astype(BF16)
        elif kind == "attn":
            attend(*t[1:])
        elif kind == "out":
            zq = {"own": zh, "p": zstep("p", 2) // 2, "n": zstep("n", 1) // 2, "far": (zh + 2) % 4}[t[1]]
            half = slice(t[2] * 256, t[2] * 256 + 256)
            for hh in range(2):
                fb = zq * 2 + hh
                total = None
                for cc in range(2):
                    w = wb[3, cc, fb // 4, fb % 4].reshape(512, 256)
                    part = lax.dot_general(att[cc, half, :], w, NT, preferred_element_type=F32)
                    total = part if total is None else total + part
                ob[fb, half, :] = total

    def land(t):
        kind = t[0]
        if kind == "HD":
            recv(hb.at[zh * 2 + oc, rows(z, t[1])], hd.at[t[1]])
        elif kind == "ZX":
            recv(blk(t[1], 1, yi, xi), wzs.at[t[1]])
        elif kind == "H":
            _, d, r, hh, j = t
            recv(hpiece(zstep(d, r + 1), hh, j), hr.at[side(d), r, hh, j])
        elif kind == "F":
            _, cls, m, d = t
            fa, sa, f, s = axes(cls)
            recv(blk(m, cls, step(f, flip(d)), s), wf.at[cls, m, side(d)])
        elif kind == "F2":
            _, cls, m = t
            fa, sa, f, s = axes(cls)
            recv(blk(m, cls, (f + 2) % 4, s), wf2.at[cls, m])
        elif kind == "S":
            _, cls, m, o, d = t
            fa, sa, f, s = axes(cls)
            recv(blk(m, cls, fblock(cls, o), step(s, flip(d))), ws.at[cls, m, o, side(d)])
        elif kind == "S2":
            _, cls, m, o = t
            fa, sa, f, s = axes(cls)
            recv(blk(m, cls, fblock(cls, o), (s + 2) % 4), ws2.at[cls, m, o])
        elif kind == "D":
            _, cls, m, o = t
            recv(dslice(m, cls, fblock(cls, o), oc), wd.at[cls, m, o])
        elif kind == "R":
            _, d, r, hh, j = t
            recv(rb.at[side(d), r, hh, j], rr.at[side(d), r, hh, j])

    def prep():
        own_kv.wait()
        for i in range(2):
            kvs[i] = wkv[:, i, :]
            rest.append(local(10 + i, kvs.at[i, :, lanes], wb.at[1 + i, c, zl, xi, yi]))

    def small():
        for d in rest:
            d.wait()
        for b in range(BUCKETS):
            pbs[c, b] = jnp.broadcast_to(pbv[:, b:b + 1], (8, LEN))
        lane = lax.broadcasted_iota(jnp.int32, (1, LEN), 1)
        for i in range(4):
            mks[zl, pl.ds(i, 1), :] = jnp.where(lane < lens[i], 1.0, 0.0)
        send(pbs.at[c], pbs.at[c], sm.at[0], "d")
        send(mks.at[zl], mks.at[zl], sm.at[1], "zp")

    def bias():
        recv(pbs.at[oc], sm.at[0])
        recv(mks.at[oz], sm.at[1])
        row = lax.broadcasted_iota(jnp.int32, (LEN, LEN), 0)
        lane = lax.broadcasted_iota(jnp.int32, (LEN, LEN), 1)
        rel = lane - row
        dist = jnp.abs(rel)
        bucket = jnp.where(rel > 0, BUCKETS // 2, 0)
        for t in STEPS:
            bucket = bucket + jnp.where(dist >= t, 1, 0)

        def bias_head(i, _):
            cc, h = i // 4, i % 4
            tab = jnp.zeros((LEN, LEN), F32)
            for b in range(BUCKETS):
                tab = jnp.where(bucket == b, pbs[cc, b, pl.ds(zl * 4 + h, 1), :], tab)
            bt[cc, pl.ds(pl.multiple_of(h * LEN, LEN), LEN), :] = tab
            return 0

        lax.fori_loop(0, 8, bias_head, 0)

    def norm(j):
        def norm_rows(i, _):
            at = pl.ds(pl.multiple_of(i * 16, 16), 16)
            total = jnp.zeros((16, 512), F32)
            for fb in range(8):
                v = hb[fb, at, :].astype(F32)
                total = total + v * v
            ms = jnp.sum(total, axis=-1, keepdims=True) * (1.0 / 4096.0)
            scale = lax.rsqrt(ms + EPS)
            for fb in range(8):
                v = hb[fb, at, :].astype(F32)
                nb[at, fb * 512:(fb + 1) * 512] = (
                    v * scale * g_ref[:, fb * 512:(fb + 1) * 512]).astype(BF16)
            return 0

        lax.fori_loop(j * 16, j * 16 + 16, norm_rows, 0)

    def attend(q, cc, j):
        head = lax.broadcasted_iota(jnp.int32, (LEN, 256), 1) // DH
        who = c if cc == 0 else oc
        at = slice((j * 2 + q) * LEN, (j * 2 + q + 1) * LEN)
        qq, kk, v = qkv[0, who, at, :], qkv[1, who, at, :], qkv[2, who, at, :]
        zero = jnp.zeros((), BF16)
        qm = jnp.concatenate([jnp.where(head == h, qq, zero) for h in range(4)], axis=0)
        s = lax.dot_general(qm, kk, NT, preferred_element_type=F32) + bt[who]
        seen = mks[q, pl.ds(2 * c + j, 1), :]
        s = jnp.where(seen > 0.5, s, -1e30)
        top = jnp.max(s, axis=-1, keepdims=True)
        e = jnp.exp(s - top)
        w = (e / jnp.sum(e, axis=-1, keepdims=True)).astype(BF16)
        mix = jnp.dot(w, v, preferred_element_type=F32)
        out = jnp.zeros((LEN, 256), F32)
        for h in range(4):
            out = jnp.where(head == h, mix[h * LEN:(h + 1) * LEN], out)
        att[who, at, :] = out.astype(BF16)

    tasks, order, _, _ = list_schedule()
    landed = set()
    for t in order:
        for n in tasks[t][2]:
            if tasks[n][0] and n not in landed:
                land(n)
                landed.add(n)
        gate(t)
        issue(t)
    for t in order:
        if tasks[t][0] and t[0] != "fin" and t not in landed:
            land(t)
    for j in range(2):
        recv(fr.at[j], fin.at[j])
        o_ref[pl.ds((oc * 2 + j) * LEN, LEN), :] = fr[j]
    for d in pending:
        d.wait_send()


def local(hidden_states, norm_gain, query_weight, keyvalue_weight, output_weight,
          position_bias, lengths):
    vm = pl.BlockSpec(memory_space=pltpu.VMEM)
    hbm = pl.BlockSpec(memory_space=pl.ANY)
    dma = pltpu.SemaphoreType.DMA
    return pl.pallas_call(
        kernel,
        out_shape=jax.ShapeDtypeStruct((512, 512), BF16),
        in_specs=[hbm] * 7,
        out_specs=vm,
        scratch_shapes=[
            pltpu.VMEM((4, 2, 2, 4, 4, 128, 256), BF16),
            pltpu.VMEM((8, 512, 512), BF16),
            pltpu.VMEM((512, 4096), BF16),
            pltpu.VMEM((3, 2, 512, 256), BF16),
            pltpu.VMEM((2, 512, 256), BF16),
            pltpu.VMEM((8, 512, 512), F32),
            pltpu.VMEM((2, 4, 2, 2, 128, 512), BF16),
            pltpu.VMEM((2, 4, 2, 2, 128, 512), BF16),
            pltpu.VMEM((2, 512, 128), F32),
            pltpu.VMEM((2, BUCKETS, 8, LEN), F32),
            pltpu.VMEM((2, 8, LEN), F32),
            pltpu.VMEM((2, 128, 512), BF16),
            pltpu.VMEM((2, 128, 512), BF16),
            pltpu.VMEM((128, 512), BF16),
            pltpu.VMEM((128, 512), BF16),
            pltpu.VMEM((128, 2, 512), BF16),
            pltpu.VMEM((2, 128, 512), BF16),
            pltpu.VMEM((1, 4096), F32),
            pltpu.VMEM((8, BUCKETS), F32),
            pltpu.SMEM((4,), jnp.int32),
            dma((12,)),
            dma((1,)),
            dma((2, 4, 2, 2)),
            dma((2,)),
            dma((4,)),
            dma((2, 4, 2)),
            dma((2, 4)),
            dma((2, 4, 4, 2)),
            dma((2, 4, 4)),
            dma((2, 4, 4)),
            dma((2, 4, 2, 2)),
            dma((2,)),
            dma((2,)),
        ],
        compiler_params=pltpu.CompilerParams(
            collective_id=0, has_side_effects=True, vmem_limit_bytes=60 * 1024 * 1024),
        name="t5_attention",
    )(hidden_states, norm_gain, query_weight[0], keyvalue_weight[0], output_weight[0],
      jnp.transpose(position_bias[0]), lengths)


def solution(mesh):
    in_specs = (
        P("dp", "mp"),
        P(),
        P(None, "dp", "mp"),
        P(None, "dp", None, "mp"),
        P(None, "dp", "mp"),
        P(None, None, "mp"),
        P("dp"),
    )
    return jax.shard_map(local, mesh=mesh, in_specs=in_specs, out_specs=P("dp", "mp"), check_vma=False)
```

```python
import functools

import jax
import jax.numpy as jnp
import numpy as np
from jax import lax
from jax.experimental import pallas as pl
from jax.experimental.pallas import tpu as pltpu
from jax.sharding import PartitionSpec as P

MESH = pl.DeviceIdType.MESH
DH = 64
BUCKETS = 32
DIST = 128
LEN = 128
EPS = 1e-06
F32 = jnp.float32
BF16 = jnp.bfloat16
NT = (((1,), (1,)), ((), ()))


def far_steps():
    half = BUCKETS // 2
    exact = half // 2
    distance = np.arange(LEN)
    scaled = np.log(np.maximum(distance, 1) / exact) / np.log(DIST / exact) * (half - exact)
    far = np.minimum(exact + np.floor(scaled + 1e-09).astype(np.int32), half - 1)
    near = np.where(distance < exact, distance, far)
    return [int(np.min(distance[near >= b])) for b in range(1, half) if np.any(near >= b)]


STEPS = far_steps()


LINKS = ("x+", "x-", "y+", "y-", "zp", "zn", "d")
RATE = {"d": 400e3}
COST = {"norm": 0.45, "proj": 0.65, "attn": 0.35, "out": 0.4, "bias": 0.5, "rs": 0.2, "fin": 0.3,
        "prep": 1.0, "small": 0.4}
AHEAD = 2.5


H_HOPS = {(0, 0): 3, (1, 0): 4, (0, 1): 3, (1, 1): 4}
R_HOPS = {(0, 0): 4, (1, 0): 3, (0, 1): 4, (1, 1): 3}


def flip(d):
    return {"+": "-", "-": "+", "p": "n", "n": "p"}[d]


def rounds(hops, d, r):
    side = d if r % 2 == 0 else flip(d)
    return hops if side == "p" else 7 - hops


OUT_NEED = {("p", 0): ("own",), ("p", 1): ("p",), ("p", 2): ("p",), ("p", 3): ("far",),
            ("n", 0): ("n",), ("n", 1): ("n",), ("n", 2): ("far",), ("n", 3): ("far",)}
RANK = {'zx': (-42.1, 18.4, 22.7, 26.7), 'h': (31.9, 45.6), 'w': (-50.6, 24.8, 11.1, 30.3), 'f': -2.0, 's0': -21.4, 's1': 7.3, 's3': 14.1, 'f2': -69.7, 's2': -40.6, 'r': -5.8}


def make_tasks():
    tasks = {}

    def add(tid, link, kib, needs, rank):
        tasks[tid] = (link, kib, tuple(needs), rank)

    add(("prep",), None, 0, (), 0.2)
    add(("small",), None, 0, [("prep",)], 30)
    for j in range(2):
        add(("HD", j), "d", 128, (), 0)
    for m in range(4):
        add(("ZX", m), "zp", 64, [("prep",)] if m in (1, 2) else (), RANK["zx"][m])
    for j in range(2):
        for d in "pn":
            for r in range(4):
                for hh in range(2):
                    if r >= rounds(H_HOPS[hh, j], d, r):
                        continue
                    need = [("HD", j)] if r == 0 and hh == 1 else []
                    if r > 0:
                        need = [("H", flip(d), r - 1, hh, j)]
                    add(("H", d, r, hh, j), "z" + d, 128, need, RANK["h"][j] + r)
    for m in range(4):
        late = RANK["w"][m]
        for cls in range(2):
            fa, sa = ("x", "y") if cls == 0 else ("y", "x")
            base = [("ZX", m)] if cls else [("prep",)] if m in (1, 2) else []
            for d in "+-":
                add(("F", cls, m, d), fa + d, 64, base, late + RANK["f"])
                add(("S", cls, m, 0, d), sa + d, 64, base, late + RANK["s0"])
                add(("S", cls, m, 1, d), sa + d, 64, [("F", cls, m, "+")], late + RANK["s1"])
                add(("S", cls, m, 2, d), sa + d, 64, [("F", cls, m, "-")], late + RANK["s1"])
                add(("S", cls, m, 3, d), sa + d, 64, [("F2", cls, m)], late + RANK["s3"])
            d = "+-"[(m + cls) % 2]
            add(("F2", cls, m), fa + d, 64, [("F", cls, m, d)], late + RANK["f2"])
            for o in range(4):
                d = "+-"[(m + cls + o) % 2]
                add(("S2", cls, m, o), sa + d, 64, [("S", cls, m, o, d)], late + RANK["s2"])
                add(("D", cls, m, o), "d", 256,
                    [("S", cls, m, o, "+"), ("S", cls, m, o, "-"), ("S2", cls, m, o)]
                    + ([("small",)] if o == 0 else []), late)

    def mine(m):
        return ([("ZX", m)] + [("F", c, m, d) for c in range(2) for d in "+-"]
                + [("F2", c, m) for c in range(2)]
                + [("S", c, m, o, d) for c in range(2) for o in range(4) for d in "+-"]
                + [("S2", c, m, o) for c in range(2) for o in range(4)])

    def theirs(m):
        return [("D", c, m, o) for c in range(2) for o in range(4)]

    for i in range(4):
        add(("bias", i), None, 0, [("small",)], 60)
    for j in range(2):
        pieces = [("HD", j)] + [t for t in tasks if t[0] == "H" and t[4] == j]
        for i in range(4):
            add(("norm", j, i), None, 0, pieces, 40 + j)
        normed = [("norm", j, i) for i in range(4)] + [("small",)]
        for m in range(3):
            add(("proj", m, 0, j), None, 0, normed + mine(m), 42 + 20 * j + 2 * m)
            add(("proj", m, 1, j), None, 0, normed + theirs(m), 43 + 20 * j + 2 * m)
        for cc in range(2):
            for q in range(2):
                add(("attn", q, cc, j), None, 0,
                    [("bias", i) for i in range(4)] + [("proj", m, cc, j) for m in range(3)], 48 + 20 * j)
        for n, step in enumerate(("far", "n", "p", "own")):
            add(("out", step, j), None, 0,
                [("attn", q, cc, j) for q in range(2) for cc in range(2)] + mine(3) + theirs(3),
                50 + 20 * j + n)
        for d in "pn":
            for r in range(4):
                for hh in range(2):
                    hops = rounds(R_HOPS[hh, j], d, r)
                    if r >= hops:
                        continue
                    need = [("out", step, j) for step in (OUT_NEED[d, r])]
                    if r < hops - 1:
                        need.append(("R", flip(d), r + 1, hh, j))
                    add(("R", d, r, hh, j), "z" + d, 128, need, 33 + RANK["r"] * j - r)
        for hh in (1, 0):
            add(("fin", hh, j), "d" if hh else None, 128,
                [("out", "own", j), ("R", "p", 0, hh, j), ("R", "n", 0, hh, j)], 30 + j)
    return tasks


def list_schedule():
    tasks = make_tasks()
    free = dict.fromkeys(LINKS, 0.0)
    arrive, finished, order = {}, {}, []
    left = dict(tasks)
    now = 0.0

    def ready_at(tid):
        t = 0.0
        for n in tasks[tid][2]:
            when = arrive.get(n) if tasks[n][0] else finished.get(n)
            if when is None:
                return None
            t = max(t, when)
        return t

    while left:
        best, soonest = None, None
        for tid in left:
            link, kib, _, rank = tasks[tid]
            at = ready_at(tid)
            if at is None:
                continue
            links = (link,) if link else ()
            for one in links:
                at = max(at, free[one] - AHEAD)
            if at <= now + 1e-9:
                key = (0 if link else 1, rank, str(tid))
                if best is None or key < best[0]:
                    best = (key, tid, links)
            elif soonest is None or at < soonest:
                soonest = at
        if best is None:
            now = soonest
            continue
        _, tid, links = best
        link, kib, _, _ = tasks[tid]
        kind = {"R": "rs"}.get(tid[0], tid[0])
        now += COST.get(kind, 0.06)
        finished[tid] = now
        if link:
            rate = RATE.get(link, 46.0e3) / 1.024e3
            t = max([now] + [free[one] for one in links]) + kib / rate
            for one in links:
                free[one] = t
            arrive[tid] = t + (1.0 if link == "d" else 1.8)
        order.append(tid)
        del left[tid]
    return tasks, order, finished, arrive


def kernel(x_ref, g_hbm, q_hbm, kv_hbm, ow_hbm, pb_hbm, len_hbm, o_ref,
           wb, hb, nb, qkv, att, ob, sb, rb, bt, pbs, mks, fs, fr,
           wq, wo, wkv, kvs, g_ref, pbv, lens,
           loc_sem, send_sem, hr, hd, wzs, wf, wf2, ws, ws2, wd, rr, sm, fin):
    dp = lax.axis_index("dp")
    mp = lax.axis_index("mp")
    zl, xi, yi = dp // 16, (dp // 4) % 4, dp % 4
    zh, c = mp // 2, mp % 2
    z = zh * 2 + zl
    oc = 1 - c
    oz = 1 - zl

    toward = 1 - 2 * zl

    def zstep(d, n):
        return (z + 8 + (toward if d == "p" else -toward) * n) % 8

    def dev(zz, xx, yy, cc):
        return ((zz % 2) * 16 + xx * 4 + yy, (zz // 2) * 2 + cc)

    xp, xm = (xi + 1) % 4, (xi + 3) % 4
    yp, ym = (yi + 1) % 4, (yi + 3) % 4
    devices = {
        "x+": dev(z, xp, yi, c), "x-": dev(z, xm, yi, c),
        "y+": dev(z, xi, yp, c), "y-": dev(z, xi, ym, c),
        "zp": dev(zstep("p", 1), xi, yi, c), "zn": dev(zstep("n", 1), xi, yi, c),
        "d": dev(z, xi, yi, oc),
    }
    pending = []

    def send(src, dst, sem, link):
        d = pltpu.make_async_remote_copy(
            src_ref=src, dst_ref=dst, send_sem=send_sem.at[0], recv_sem=sem,
            device_id=devices[link], device_id_type=MESH)
        d.start()
        pending.append(d)

    def recv(dst, sem):
        pltpu.make_async_remote_copy(
            src_ref=dst, dst_ref=dst, send_sem=send_sem.at[0], recv_sem=sem,
            device_id=devices["d"], device_id_type=MESH).wait_recv()

    lanes = pl.ds(pl.multiple_of(zl * 256, 256), 256)
    far_lanes = pl.ds(pl.multiple_of(oz * 256, 256), 256)

    def source(m, at):
        if m == 0:
            return wq.at[:, at]
        if m == 3:
            return wo.at[:, at]
        return kvs.at[m - 1, :, at]

    def col(zz, hh):
        return (zz // 2) * 2 + (c if hh == 0 else oc)

    def rows(zz, j):
        return pl.ds(pl.multiple_of((j * 2 + zz % 2) * LEN, LEN), LEN)

    def local(i, src, dst):
        d = pltpu.make_async_copy(src, dst, loc_sem.at[i])
        d.start()
        return d

    own_x = [local(j, x_ref.at[pl.ds((c * 2 + j) * LEN, LEN)], hb.at[mp, rows(z, j)]) for j in range(2)]
    own_q = local(2, q_hbm, wq)
    own_kv = local(3, kv_hbm, wkv)
    own_o = local(4, ow_hbm, wo)
    rest = [local(5, pb_hbm, pbv), local(6, len_hbm, lens), local(7, g_hbm, g_ref),
            local(8, q_hbm.at[:, lanes], wb.at[0, c, zl, xi, yi]),
            local(9, ow_hbm.at[:, lanes], wb.at[3, c, zl, xi, yi])]

    barrier = pltpu.get_barrier_semaphore()
    for link in LINKS:
        pl.semaphore_signal(barrier, inc=1, device_id=devices[link], device_id_type=MESH)
    pl.semaphore_wait(barrier, len(LINKS))

    def blk(m, cls, f, s):
        bx, by = (f, s) if cls == 0 else (s, f)
        return wb.at[m, c, zl if cls == 0 else oz, bx, by]

    def axes(cls):
        return ("x", "y", xi, yi) if cls == 0 else ("y", "x", yi, xi)

    def step(i, d):
        return (i + (1 if d == "+" else 3)) % 4

    def fblock(cls, o):
        f = axes(cls)[2]
        return (f + (0, 3, 1, 2)[o]) % 4

    def dslice(m, cls, ff, cc):
        if cls == 0:
            return wb.at[m, cc, zl, ff]
        return wb.at[m, cc, oz, :, ff]

    def hpiece(zo, hh, j):
        return hb.at[col(zo, hh), rows(zo, j)]

    def side(d):
        return 0 if d in "+p" else 1

    waits = {"x0": own_x[0], "x1": own_x[1], "q": own_q, "o": own_o}

    def gate(t):
        key = None
        if t[0] == "H" and t[2] == 0 and t[3] == 0:
            key = "x%d" % t[4]
        elif t[0] in ("ZX", "F", "S"):
            m = t[1] if t[0] == "ZX" else t[2]
            key = {0: "q", 3: "o"}.get(m)
        if key in waits:
            waits.pop(key).wait()

    def issue(t):
        kind = t[0]
        if kind == "HD":
            send(x_ref.at[pl.ds((oc * 2 + t[1]) * LEN, LEN)], hb.at[mp, rows(z, t[1])], hd.at[t[1]], "d")
        elif kind == "ZX":
            send(source(t[1], far_lanes), wb.at[t[1], c, zl, xi, yi], wzs.at[t[1]], "zp")
        elif kind == "H":
            _, d, r, hh, j = t
            p = hpiece(zstep(flip(d), r), hh, j)
            send(p, p, hr.at[side(d), r, hh, j], "z" + d)
        elif kind == "F":
            _, cls, m, d = t
            fa, sa, f, s = axes(cls)
            own = blk(m, cls, f, s)
            send(source(m, lanes) if cls == 0 else own, own, wf.at[cls, m, side(d)], fa + d)
        elif kind == "F2":
            _, cls, m = t
            fa, sa, f, s = axes(cls)
            d = "+-"[(m + cls) % 2]
            b = blk(m, cls, step(f, flip(d)), s)
            send(b, b, wf2.at[cls, m], fa + d)
        elif kind == "S":
            _, cls, m, o, d = t
            fa, sa, f, s = axes(cls)
            b = blk(m, cls, fblock(cls, o), s)
            send(source(m, lanes) if cls == 0 and o == 0 else b, b, ws.at[cls, m, o, side(d)], sa + d)
        elif kind == "S2":
            _, cls, m, o = t
            fa, sa, f, s = axes(cls)
            d = "+-"[(m + cls + o) % 2]
            b = blk(m, cls, fblock(cls, o), step(s, flip(d)))
            send(b, b, ws2.at[cls, m, o], sa + d)
        elif kind == "D":
            _, cls, m, o = t
            p = dslice(m, cls, fblock(cls, o), c)
            send(p, p, wd.at[cls, m, o], "d")
        elif kind == "R":
            _, d, r, hh, j = t
            dz = zstep(d, r + 1)
            value = ob[col(dz, hh), rows(dz, j), :]
            if r < rounds(R_HOPS[hh, j], d, r) - 1:
                value = value + rb[side(flip(d)), r + 1, hh, j].astype(F32)
            sb[side(d), r, hh, j] = value.astype(BF16)
            send(sb.at[side(d), r, hh, j], rb.at[side(d), r, hh, j], rr.at[side(d), r, hh, j], "z" + d)
        elif kind == "fin":
            _, hh, j = t
            value = (hb[col(z, hh), rows(z, j), :].astype(F32) + ob[col(z, hh), rows(z, j), :]
                     + rb[0, 0, hh, j].astype(F32) + rb[1, 0, hh, j].astype(F32)).astype(BF16)
            if hh:
                fs[j] = value
                send(fs.at[j], fr.at[j], fin.at[j], "d")
            else:
                o_ref[pl.ds((c * 2 + j) * LEN, LEN), :] = value
        elif kind == "prep":
            prep()
        elif kind == "small":
            small()
        elif kind == "bias":
            bias(t[1])
        elif kind == "norm":
            norm(t[1], t[2])
        elif kind == "proj":
            _, m, cc, j = t
            who = c if cc == 0 else oc
            w = wb[m, who].reshape(4096, 256)
            half = slice(j * 256, j * 256 + 256)
            qkv[m, who, half, :] = jnp.dot(
                nb[half, :], w, preferred_element_type=F32).astype(BF16)
        elif kind == "attn":
            attend(*t[1:])
        elif kind == "out":
            zq = {"own": zh, "p": zstep("p", 2) // 2, "n": zstep("n", 1) // 2, "far": (zh + 2) % 4}[t[1]]
            half = slice(t[2] * 256, t[2] * 256 + 256)
            for hh in range(2):
                fb = zq * 2 + hh
                total = None
                for cc in range(2):
                    w = wb[3, cc, fb // 4, fb % 4].reshape(512, 256)
                    part = lax.dot_general(att[cc, half, :], w, NT, preferred_element_type=F32)
                    total = part if total is None else total + part
                ob[fb, half, :] = total

    def land(t):
        kind = t[0]
        if kind == "HD":
            recv(hb.at[zh * 2 + oc, rows(z, t[1])], hd.at[t[1]])
        elif kind == "ZX":
            recv(blk(t[1], 1, yi, xi), wzs.at[t[1]])
        elif kind == "H":
            _, d, r, hh, j = t
            recv(hpiece(zstep(d, r + 1), hh, j), hr.at[side(d), r, hh, j])
        elif kind == "F":
            _, cls, m, d = t
            fa, sa, f, s = axes(cls)
            recv(blk(m, cls, step(f, flip(d)), s), wf.at[cls, m, side(d)])
        elif kind == "F2":
            _, cls, m = t
            fa, sa, f, s = axes(cls)
            recv(blk(m, cls, (f + 2) % 4, s), wf2.at[cls, m])
        elif kind == "S":
            _, cls, m, o, d = t
            fa, sa, f, s = axes(cls)
            recv(blk(m, cls, fblock(cls, o), step(s, flip(d))), ws.at[cls, m, o, side(d)])
        elif kind == "S2":
            _, cls, m, o = t
            fa, sa, f, s = axes(cls)
            recv(blk(m, cls, fblock(cls, o), (s + 2) % 4), ws2.at[cls, m, o])
        elif kind == "D":
            _, cls, m, o = t
            recv(dslice(m, cls, fblock(cls, o), oc), wd.at[cls, m, o])
        elif kind == "R":
            _, d, r, hh, j = t
            recv(rb.at[side(d), r, hh, j], rr.at[side(d), r, hh, j])

    def prep():
        own_kv.wait()
        for i in range(2):
            kvs[i] = wkv[:, i, :]
            rest.append(local(10 + i, kvs.at[i, :, lanes], wb.at[1 + i, c, zl, xi, yi]))

    def small():
        for d in rest:
            d.wait()
        for b in range(BUCKETS):
            pbs[c, b] = jnp.broadcast_to(pbv[:, b:b + 1], (8, LEN))
        lane = lax.broadcasted_iota(jnp.int32, (1, LEN), 1)
        for i in range(4):
            mks[zl, pl.ds(i, 1), :] = jnp.where(lane < lens[i], 1.0, 0.0)
        send(pbs.at[c], pbs.at[c], sm.at[0], "d")
        send(mks.at[zl], mks.at[zl], sm.at[1], "zp")

    def bias(part):
        if part == 0:
            recv(mks.at[oz], sm.at[1])
        if part == 2:
            recv(pbs.at[oc], sm.at[0])
        row = lax.broadcasted_iota(jnp.int32, (LEN, LEN), 0)
        lane = lax.broadcasted_iota(jnp.int32, (LEN, LEN), 1)
        rel = lane - row
        dist = jnp.abs(rel)
        bucket = jnp.where(rel > 0, BUCKETS // 2, 0)
        for t in STEPS:
            bucket = bucket + jnp.where(dist >= t, 1, 0)

        def bias_head(i, _):
            cc, h = c if part < 2 else oc, i % 4
            tab = jnp.zeros((LEN, LEN), F32)
            for b in range(BUCKETS):
                tab = jnp.where(bucket == b, pbs[cc, b, pl.ds(zl * 4 + h, 1), :], tab)
            bt[cc, pl.ds(pl.multiple_of(h * LEN, LEN), LEN), :] = tab
            return 0

        lax.fori_loop(part * 2, part * 2 + 2, bias_head, 0)

    def norm(j, part):
        def norm_rows(i, _):
            at = pl.ds(pl.multiple_of(i * 16, 16), 16)
            total = jnp.zeros((16, 512), F32)
            for fb in range(8):
                v = hb[fb, at, :].astype(F32)
                total = total + v * v
            ms = jnp.sum(total, axis=-1, keepdims=True) * (1.0 / 4096.0)
            scale = lax.rsqrt(ms + EPS)
            for fb in range(8):
                v = hb[fb, at, :].astype(F32)
                nb[at, fb * 512:(fb + 1) * 512] = (
                    v * scale * g_ref[:, fb * 512:(fb + 1) * 512]).astype(BF16)
            return 0

        lax.fori_loop(j * 16 + part * 4, j * 16 + part * 4 + 4, norm_rows, 0)

    def attend(q, cc, j):
        head = lax.broadcasted_iota(jnp.int32, (LEN, 256), 1) // DH
        who = c if cc == 0 else oc
        at = slice((j * 2 + q) * LEN, (j * 2 + q + 1) * LEN)
        qq, kk, v = qkv[0, who, at, :], qkv[1, who, at, :], qkv[2, who, at, :]
        zero = jnp.zeros((), BF16)
        qm = jnp.concatenate([jnp.where(head == h, qq, zero) for h in range(4)], axis=0)
        s = lax.dot_general(qm, kk, NT, preferred_element_type=F32) + bt[who]
        seen = mks[q, pl.ds(2 * c + j, 1), :]
        s = jnp.where(seen > 0.5, s, -1e30)
        top = jnp.max(s, axis=-1, keepdims=True)
        e = jnp.exp(s - top)
        w = (e / jnp.sum(e, axis=-1, keepdims=True)).astype(BF16)
        mix = jnp.dot(w, v, preferred_element_type=F32)
        out = jnp.zeros((LEN, 256), F32)
        for h in range(4):
            out = jnp.where(head == h, mix[h * LEN:(h + 1) * LEN], out)
        att[who, at, :] = out.astype(BF16)

    tasks, order, _, _ = list_schedule()
    landed = set()
    for t in order:
        for n in tasks[t][2]:
            if tasks[n][0] and n not in landed:
                land(n)
                landed.add(n)
        gate(t)
        issue(t)
    for t in order:
        if tasks[t][0] and t[0] != "fin" and t not in landed:
            land(t)
    for j in range(2):
        recv(fr.at[j], fin.at[j])
        o_ref[pl.ds((oc * 2 + j) * LEN, LEN), :] = fr[j]
    for d in pending:
        d.wait_send()


def local(hidden_states, norm_gain, query_weight, keyvalue_weight, output_weight,
          position_bias, lengths):
    vm = pl.BlockSpec(memory_space=pltpu.VMEM)
    hbm = pl.BlockSpec(memory_space=pl.ANY)
    dma = pltpu.SemaphoreType.DMA
    return pl.pallas_call(
        kernel,
        out_shape=jax.ShapeDtypeStruct((512, 512), BF16),
        in_specs=[hbm] * 7,
        out_specs=vm,
        scratch_shapes=[
            pltpu.VMEM((4, 2, 2, 4, 4, 128, 256), BF16),
            pltpu.VMEM((8, 512, 512), BF16),
            pltpu.VMEM((512, 4096), BF16),
            pltpu.VMEM((3, 2, 512, 256), BF16),
            pltpu.VMEM((2, 512, 256), BF16),
            pltpu.VMEM((8, 512, 512), F32),
            pltpu.VMEM((2, 4, 2, 2, 128, 512), BF16),
            pltpu.VMEM((2, 4, 2, 2, 128, 512), BF16),
            pltpu.VMEM((2, 512, 128), F32),
            pltpu.VMEM((2, BUCKETS, 8, LEN), F32),
            pltpu.VMEM((2, 8, LEN), F32),
            pltpu.VMEM((2, 128, 512), BF16),
            pltpu.VMEM((2, 128, 512), BF16),
            pltpu.VMEM((128, 512), BF16),
            pltpu.VMEM((128, 512), BF16),
            pltpu.VMEM((128, 2, 512), BF16),
            pltpu.VMEM((2, 128, 512), BF16),
            pltpu.VMEM((1, 4096), F32),
            pltpu.VMEM((8, BUCKETS), F32),
            pltpu.SMEM((4,), jnp.int32),
            dma((12,)),
            dma((1,)),
            dma((2, 4, 2, 2)),
            dma((2,)),
            dma((4,)),
            dma((2, 4, 2)),
            dma((2, 4)),
            dma((2, 4, 4, 2)),
            dma((2, 4, 4)),
            dma((2, 4, 4)),
            dma((2, 4, 2, 2)),
            dma((2,)),
            dma((2,)),
        ],
        compiler_params=pltpu.CompilerParams(
            collective_id=0, has_side_effects=True, vmem_limit_bytes=60 * 1024 * 1024),
        name="t5_attention",
    )(hidden_states, norm_gain, query_weight[0], keyvalue_weight[0], output_weight[0],
      jnp.transpose(position_bias[0]), lengths)


def solution(mesh):
    in_specs = (
        P("dp", "mp"),
        P(),
        P(None, "dp", "mp"),
        P(None, "dp", None, "mp"),
        P(None, "dp", "mp"),
        P(None, None, "mp"),
        P("dp"),
    )
    return jax.shard_map(local, mesh=mesh, in_specs=in_specs, out_specs=P("dp", "mp"), check_vma=False)
```

```python
import functools

import jax
import jax.numpy as jnp
import numpy as np
from jax import lax
from jax.experimental import pallas as pl
from jax.experimental.pallas import tpu as pltpu
from jax.sharding import PartitionSpec as P

MESH = pl.DeviceIdType.MESH
DH = 64
BUCKETS = 32
DIST = 128
LEN = 128
EPS = 1e-06
F32 = jnp.float32
BF16 = jnp.bfloat16
NT = (((1,), (1,)), ((), ()))


def far_steps():
    half = BUCKETS // 2
    exact = half // 2
    distance = np.arange(LEN)
    scaled = np.log(np.maximum(distance, 1) / exact) / np.log(DIST / exact) * (half - exact)
    far = np.minimum(exact + np.floor(scaled + 1e-09).astype(np.int32), half - 1)
    near = np.where(distance < exact, distance, far)
    return [int(np.min(distance[near >= b])) for b in range(1, half) if np.any(near >= b)]


STEPS = far_steps()


LINKS = ("x+", "x-", "y+", "y-", "zp", "zn", "d")
RATE = {"d": 500e3}
COST = {"norm": 0.45, "proj": 0.65, "soft": 0.28, "attn": 0.12, "out": 0.4, "bias": 0.5, "rs": 0.2, "fin": 0.3,
        "prep": 1.0, "small": 0.4}
AHEAD = 2.7
HOLD = 0.1


H_HOPS = {(0, 0): 3, (1, 0): 4, (0, 1): 3, (1, 1): 4}
R_HOPS = {(0, 0): 4, (1, 0): 3, (0, 1): 3, (1, 1): 4}


def flip(d):
    return {"+": "-", "-": "+", "p": "n", "n": "p"}[d]


def rounds(hops, d, r):
    side = d if r % 2 == 0 else flip(d)
    return hops if side == "p" else 7 - hops


OUT_NEED = {("p", 0): ("own",), ("p", 1): ("p",), ("p", 2): ("p",), ("p", 3): ("far",),
            ("n", 0): ("n",), ("n", 1): ("n",), ("n", 2): ("far",), ("n", 3): ("far",)}
RANK = {'zx': (-62.8, -38.1, 16.7, -3.3), 'h': (22.2, 71.8), 'w': (1.9, 27.0, 3.6, 30.5), 'f': -8.7, 's0': -46.4, 's1': 5.5, 's3': 28.7, 'f2': -21.6, 's2': -36.9, 'r': -21.5}


def make_tasks():
    tasks = {}

    def add(tid, link, kib, needs, rank):
        tasks[tid] = (link, kib, tuple(needs), rank)

    add(("prep",), None, 0, (), 0.2)
    add(("small",), None, 0, [("prep",)], 30)
    for j in range(2):
        add(("HD", j), "d", 128, (), 0)
    for m in range(4):
        add(("ZX", m), "zp", 64, [("prep",)] if m in (1, 2) else (), RANK["zx"][m])
    for j in range(2):
        for d in "pn":
            for r in range(4):
                for hh in range(2):
                    if r >= rounds(H_HOPS[hh, j], d, r):
                        continue
                    need = [("HD", j)] if r == 0 and hh == 1 else []
                    if r > 0:
                        need = [("H", flip(d), r - 1, hh, j)]
                    add(("H", d, r, hh, j), "z" + d, 128, need, RANK["h"][j] + r)
    for m in range(4):
        late = RANK["w"][m]
        for cls in range(2):
            fa, sa = ("x", "y") if cls == 0 else ("y", "x")
            base = [("ZX", m)] if cls else [("prep",)] if m in (1, 2) else []
            for d in "+-":
                add(("F", cls, m, d), fa + d, 64, base, late + RANK["f"])
                add(("S", cls, m, 0, d), sa + d, 64, base, late + RANK["s0"])
                add(("S", cls, m, 1, d), sa + d, 64, [("F", cls, m, "+")], late + RANK["s1"])
                add(("S", cls, m, 2, d), sa + d, 64, [("F", cls, m, "-")], late + RANK["s1"])
                add(("S", cls, m, 3, d), sa + d, 64, [("F2", cls, m)], late + RANK["s3"])
            d = "+-"[(m + cls) % 2]
            add(("F2", cls, m), fa + d, 64, [("F", cls, m, d)], late + RANK["f2"])
            for o in range(4):
                d = "+-"[(m + cls + o) % 2]
                add(("S2", cls, m, o), sa + d, 64, [("S", cls, m, o, d)], late + RANK["s2"])
                if o < 3:
                    add(("D", cls, m, o), "d", 256,
                        [("S", cls, m, o, "+"), ("S", cls, m, o, "-"), ("S2", cls, m, o)]
                        + ([("small",)] if o == 0 else []), late)
                    continue
                for i, need in enumerate((("F2", cls, m), ("S", cls, m, o, "+"), ("S", cls, m, o, "-"), ("S2", cls, m, o))):
                    add(("D", cls, m, o + i), "d", 64, [need], late)

    def mine(m):
        return ([("ZX", m)] + [("F", c, m, d) for c in range(2) for d in "+-"]
                + [("F2", c, m) for c in range(2)]
                + [("S", c, m, o, d) for c in range(2) for o in range(4) for d in "+-"]
                + [("S2", c, m, o) for c in range(2) for o in range(4)])

    def theirs(m):
        return [("D", c, m, o) for c in range(2) for o in range(7)]

    for i in range(4):
        add(("bias", i), None, 0, [("small",)], 60)
    for j in range(2):
        pieces = [("HD", j)] + [t for t in tasks if t[0] == "H" and t[4] == j]
        for i in range(4):
            add(("norm", j, i), None, 0, pieces, 40 + j)
        normed = [("norm", j, i) for i in range(4)] + [("small",)]
        for m in range(3):
            add(("proj", m, 0, j), None, 0, normed + mine(m), 42 + 20 * j + 2 * m)
            add(("proj", m, 1, j), None, 0, normed + theirs(m), 43 + 20 * j + 2 * m)
        for cc in range(2):
            for q in range(2):
                add(("soft", q, cc, j), None, 0,
                    [("bias", i) for i in range(4)] + [("proj", m, cc, j) for m in range(2)], 48 + 20 * j)
                add(("attn", q, cc, j), None, 0, [("soft", q, cc, j), ("proj", 2, cc, j)], 48 + 20 * j)
        for n, step in enumerate(("far", "n", "p", "own")):
            add(("out", step, j), None, 0,
                [("attn", q, cc, j) for q in range(2) for cc in range(2)] + mine(3) + theirs(3),
                50 + 20 * j + n)
        for d in "pn":
            for r in range(4):
                for hh in range(2):
                    hops = rounds(R_HOPS[hh, j], d, r)
                    if r >= hops:
                        continue
                    need = [("out", step, j) for step in (OUT_NEED[d, r])]
                    if r < hops - 1:
                        need.append(("R", flip(d), r + 1, hh, j))
                    add(("R", d, r, hh, j), "z" + d, 128, need, 33 + RANK["r"] * j - r)
        for hh in (1, 0):
            add(("fin", hh, j), "d" if hh else None, 128,
                [("out", "own", j), ("R", "p", 0, hh, j), ("R", "n", 0, hh, j)], 30 + j)
    return tasks


def list_schedule():
    tasks = make_tasks()
    free = dict.fromkeys(LINKS, 0.0)
    arrive, finished, order = {}, {}, []
    left = dict(tasks)
    now, summing = 0.0, False

    def ready_at(tid):
        t = 0.0
        for n in tasks[tid][2]:
            when = arrive.get(n) if tasks[n][0] else finished.get(n)
            if when is None:
                return None
            t = max(t, when)
        return t

    while left:
        best, soonest, due = None, None, None
        for tid in left:
            link, kib, _, rank = tasks[tid]
            at = ready_at(tid)
            if at is None:
                continue
            links = (link,) if link else ()
            for one in links:
                at = max(at, free[one] - AHEAD)
            if at <= now + 1e-9:
                key = (0 if link else 1, rank, str(tid))
                if best is None or key < best[0]:
                    best = (key, tid, links)
            else:
                soonest = at if soonest is None else min(at, soonest)
                if link:
                    due = at if due is None else min(at, due)
        if best is None:
            now = soonest
            continue
        _, tid, links = best
        if summing and not links and due is not None and due < now + COST.get(tid[0], 0.06) - HOLD:
            now = due
            continue
        summing = summing or tid[0] == "R"
        link, kib, _, _ = tasks[tid]
        kind = {"R": "rs"}.get(tid[0], tid[0])
        now += COST.get(kind, 0.06)
        finished[tid] = now
        if link:
            rate = RATE.get(link, 46.0e3) / 1.024e3
            t = max([now] + [free[one] for one in links]) + kib / rate
            for one in links:
                free[one] = t
            arrive[tid] = t + (1.0 if link == "d" else 1.8)
        order.append(tid)
        del left[tid]
    return tasks, order, finished, arrive


def kernel(x_ref, g_hbm, q_hbm, kv_hbm, ow_hbm, pb_hbm, len_hbm, o_ref,
           wb, hb, nb, qkv, att, ob, sb, rb, bt, pbs, mks, fs, fr, wts,
           wq, wo, wkv, kvs, g_ref, pbv, lens,
           loc_sem, send_sem, hr, hd, wzs, wf, wf2, ws, ws2, wd, rr, sm, fin):
    dp = lax.axis_index("dp")
    mp = lax.axis_index("mp")
    zl, xi, yi = dp // 16, (dp // 4) % 4, dp % 4
    zh, c = mp // 2, mp % 2
    z = zh * 2 + zl
    oc = 1 - c
    oz = 1 - zl

    toward = 1 - 2 * zl

    def zstep(d, n):
        return (z + 8 + (toward if d == "p" else -toward) * n) % 8

    def dev(zz, xx, yy, cc):
        return ((zz % 2) * 16 + xx * 4 + yy, (zz // 2) * 2 + cc)

    xp, xm = (xi + 1) % 4, (xi + 3) % 4
    yp, ym = (yi + 1) % 4, (yi + 3) % 4
    devices = {
        "x+": dev(z, xp, yi, c), "x-": dev(z, xm, yi, c),
        "y+": dev(z, xi, yp, c), "y-": dev(z, xi, ym, c),
        "zp": dev(zstep("p", 1), xi, yi, c), "zn": dev(zstep("n", 1), xi, yi, c),
        "d": dev(z, xi, yi, oc),
    }
    pending, outs = [], []

    def send(src, dst, sem, link):
        d = pltpu.make_async_remote_copy(
            src_ref=src, dst_ref=dst, send_sem=send_sem.at[0], recv_sem=sem,
            device_id=devices[link], device_id_type=MESH)
        d.start()
        pending.append(d)

    def recv(dst, sem):
        pltpu.make_async_remote_copy(
            src_ref=dst, dst_ref=dst, send_sem=send_sem.at[0], recv_sem=sem,
            device_id=devices["d"], device_id_type=MESH).wait_recv()

    lanes = pl.ds(pl.multiple_of(zl * 256, 256), 256)
    far_lanes = pl.ds(pl.multiple_of(oz * 256, 256), 256)

    def source(m, at):
        if m == 0:
            return wq.at[:, at]
        if m == 3:
            return wo.at[:, at]
        return kvs.at[m - 1, :, at]

    def col(zz, hh):
        return (zz // 2) * 2 + (c if hh == 0 else oc)

    def rows(zz, j):
        return pl.ds(pl.multiple_of((j * 2 + zz % 2) * LEN, LEN), LEN)

    def local(i, src, dst):
        d = pltpu.make_async_copy(src, dst, loc_sem.at[i])
        d.start()
        return d

    own_x = [local(j, x_ref.at[pl.ds((c * 2 + j) * LEN, LEN)], hb.at[mp, rows(z, j)]) for j in range(2)]
    own_q = local(2, q_hbm, wq)
    own_kv = local(3, kv_hbm, wkv)
    own_o = local(4, ow_hbm, wo)
    rest = [local(5, pb_hbm, pbv), local(6, len_hbm, lens), local(7, g_hbm, g_ref),
            local(8, q_hbm.at[:, lanes], wb.at[0, c, zl, xi, yi]),
            local(9, ow_hbm.at[:, lanes], wb.at[3, c, zl, xi, yi])]

    barrier = pltpu.get_barrier_semaphore()
    for link in LINKS:
        pl.semaphore_signal(barrier, inc=1, device_id=devices[link], device_id_type=MESH)
    pl.semaphore_wait(barrier, len(LINKS))

    def blk(m, cls, f, s):
        bx, by = (f, s) if cls == 0 else (s, f)
        return wb.at[m, c, zl if cls == 0 else oz, bx, by]

    def axes(cls):
        return ("x", "y", xi, yi) if cls == 0 else ("y", "x", yi, xi)

    def step(i, d):
        return (i + (1 if d == "+" else 3)) % 4

    def fblock(cls, o):
        f = axes(cls)[2]
        return (f + (0, 3, 1, 2)[o]) % 4

    def dslice(m, cls, o, cc):
        f, s = axes(cls)[2:]
        ff = fblock(cls, min(o, 3))
        if o >= 3:
            s = (s + (0, 3, 1, 2)[o - 3]) % 4
            bx, by = (ff, s) if cls == 0 else (s, ff)
            return wb.at[m, cc, zl if cls == 0 else oz, bx, by]
        if cls == 0:
            return wb.at[m, cc, zl, ff]
        return wb.at[m, cc, oz, :, ff]

    def hpiece(zo, hh, j):
        return hb.at[col(zo, hh), rows(zo, j)]

    def side(d):
        return 0 if d in "+p" else 1

    waits = {"x0": own_x[0], "x1": own_x[1], "q": own_q, "o": own_o}

    def gate(t):
        key = None
        if t[0] == "H" and t[2] == 0 and t[3] == 0:
            key = "x%d" % t[4]
        elif t[0] in ("ZX", "F", "S"):
            m = t[1] if t[0] == "ZX" else t[2]
            key = {0: "q", 3: "o"}.get(m)
        if key in waits:
            waits.pop(key).wait()

    def issue(t):
        kind = t[0]
        if kind == "HD":
            send(x_ref.at[pl.ds((oc * 2 + t[1]) * LEN, LEN)], hb.at[mp, rows(z, t[1])], hd.at[t[1]], "d")
        elif kind == "ZX":
            send(source(t[1], far_lanes), wb.at[t[1], c, zl, xi, yi], wzs.at[t[1]], "zp")
        elif kind == "H":
            _, d, r, hh, j = t
            p = hpiece(zstep(flip(d), r), hh, j)
            send(p, p, hr.at[side(d), r, hh, j], "z" + d)
        elif kind == "F":
            _, cls, m, d = t
            fa, sa, f, s = axes(cls)
            own = blk(m, cls, f, s)
            send(source(m, lanes) if cls == 0 else own, own, wf.at[cls, m, side(d)], fa + d)
        elif kind == "F2":
            _, cls, m = t
            fa, sa, f, s = axes(cls)
            d = "+-"[(m + cls) % 2]
            b = blk(m, cls, step(f, flip(d)), s)
            send(b, b, wf2.at[cls, m], fa + d)
        elif kind == "S":
            _, cls, m, o, d = t
            fa, sa, f, s = axes(cls)
            b = blk(m, cls, fblock(cls, o), s)
            send(source(m, lanes) if cls == 0 and o == 0 else b, b, ws.at[cls, m, o, side(d)], sa + d)
        elif kind == "S2":
            _, cls, m, o = t
            fa, sa, f, s = axes(cls)
            d = "+-"[(m + cls + o) % 2]
            b = blk(m, cls, fblock(cls, o), step(s, flip(d)))
            send(b, b, ws2.at[cls, m, o], sa + d)
        elif kind == "D":
            _, cls, m, o = t
            p = dslice(m, cls, o, c)
            send(p, p, wd.at[cls, m, o], "d")
        elif kind == "R":
            _, d, r, hh, j = t
            dz = zstep(d, r + 1)
            value = ob[col(dz, hh), rows(dz, j), :]
            if r < rounds(R_HOPS[hh, j], d, r) - 1:
                value = value + rb[side(flip(d)), r + 1, hh, j].astype(F32)
            sb[side(d), r, hh, j] = value.astype(BF16)
            send(sb.at[side(d), r, hh, j], rb.at[side(d), r, hh, j], rr.at[side(d), r, hh, j], "z" + d)
        elif kind == "fin":
            _, hh, j = t
            value = (hb[col(z, hh), rows(z, j), :].astype(F32) + ob[col(z, hh), rows(z, j), :]
                     + rb[0, 0, hh, j].astype(F32) + rb[1, 0, hh, j].astype(F32)).astype(BF16)
            if hh:
                fs[j] = value
                send(fs.at[j], o_ref.at[pl.ds((c * 2 + j) * LEN, LEN)], fin.at[j], "d")
            else:
                fr[j] = value
                outs.append(local(12 + j, fr.at[j], o_ref.at[pl.ds((c * 2 + j) * LEN, LEN)]))
        elif kind == "prep":
            prep()
        elif kind == "small":
            small()
        elif kind == "bias":
            bias(t[1])
        elif kind == "norm":
            norm(t[1], t[2])
        elif kind == "proj":
            _, m, cc, j = t
            who = c if cc == 0 else oc
            w = wb[m, who].reshape(4096, 256)
            half = slice(j * 256, j * 256 + 256)
            qkv[m, who, half, :] = jnp.dot(
                nb[half, :], w, preferred_element_type=F32).astype(BF16)
        elif kind == "soft":
            soften(*t[1:])
        elif kind == "attn":
            attend(*t[1:])
        elif kind == "out":
            zq = {"own": zh, "p": zstep("p", 2) // 2, "n": zstep("n", 1) // 2, "far": (zh + 2) % 4}[t[1]]
            half = slice(t[2] * 256, t[2] * 256 + 256)
            for hh in range(2):
                fb = zq * 2 + hh
                total = None
                for cc in range(2):
                    w = wb[3, cc, fb // 4, fb % 4].reshape(512, 256)
                    part = lax.dot_general(att[cc, half, :], w, NT, preferred_element_type=F32)
                    total = part if total is None else total + part
                ob[fb, half, :] = total

    def land(t):
        kind = t[0]
        if kind == "HD":
            recv(hb.at[zh * 2 + oc, rows(z, t[1])], hd.at[t[1]])
        elif kind == "ZX":
            recv(blk(t[1], 1, yi, xi), wzs.at[t[1]])
        elif kind == "H":
            _, d, r, hh, j = t
            recv(hpiece(zstep(d, r + 1), hh, j), hr.at[side(d), r, hh, j])
        elif kind == "F":
            _, cls, m, d = t
            fa, sa, f, s = axes(cls)
            recv(blk(m, cls, step(f, flip(d)), s), wf.at[cls, m, side(d)])
        elif kind == "F2":
            _, cls, m = t
            fa, sa, f, s = axes(cls)
            recv(blk(m, cls, (f + 2) % 4, s), wf2.at[cls, m])
        elif kind == "S":
            _, cls, m, o, d = t
            fa, sa, f, s = axes(cls)
            recv(blk(m, cls, fblock(cls, o), step(s, flip(d))), ws.at[cls, m, o, side(d)])
        elif kind == "S2":
            _, cls, m, o = t
            fa, sa, f, s = axes(cls)
            recv(blk(m, cls, fblock(cls, o), (s + 2) % 4), ws2.at[cls, m, o])
        elif kind == "D":
            _, cls, m, o = t
            recv(dslice(m, cls, o, oc), wd.at[cls, m, o])
        elif kind == "R":
            _, d, r, hh, j = t
            recv(rb.at[side(d), r, hh, j], rr.at[side(d), r, hh, j])

    def prep():
        own_kv.wait()
        for i in range(2):
            kvs[i] = wkv[:, i, :]
            rest.append(local(10 + i, kvs.at[i, :, lanes], wb.at[1 + i, c, zl, xi, yi]))

    def small():
        for d in rest:
            d.wait()
        for b in range(BUCKETS):
            pbs[c, b] = jnp.broadcast_to(pbv[:, b:b + 1], (8, LEN))
        lane = lax.broadcasted_iota(jnp.int32, (1, LEN), 1)
        for i in range(4):
            mks[zl, pl.ds(i, 1), :] = jnp.where(lane < lens[i], 1.0, 0.0)
        send(pbs.at[c], pbs.at[c], sm.at[0], "d")
        send(mks.at[zl], mks.at[zl], sm.at[1], "zp")

    def bias(part):
        if part == 0:
            recv(mks.at[oz], sm.at[1])
        if part == 2:
            recv(pbs.at[oc], sm.at[0])
        row = lax.broadcasted_iota(jnp.int32, (LEN, LEN), 0)
        lane = lax.broadcasted_iota(jnp.int32, (LEN, LEN), 1)
        rel = lane - row
        dist = jnp.abs(rel)
        bucket = jnp.where(rel > 0, BUCKETS // 2, 0)
        for t in STEPS:
            bucket = bucket + jnp.where(dist >= t, 1, 0)

        def bias_head(i, _):
            cc, h = c if part < 2 else oc, i % 4
            tab = jnp.zeros((LEN, LEN), F32)
            for b in range(BUCKETS):
                tab = jnp.where(bucket == b, pbs[cc, b, pl.ds(zl * 4 + h, 1), :], tab)
            bt[cc, pl.ds(pl.multiple_of(h * LEN, LEN), LEN), :] = tab
            return 0

        lax.fori_loop(part * 2, part * 2 + 2, bias_head, 0)

    def norm(j, part):
        def norm_rows(i, _):
            at = pl.ds(pl.multiple_of(i * 16, 16), 16)
            total = jnp.zeros((16, 512), F32)
            for fb in range(8):
                v = hb[fb, at, :].astype(F32)
                total = total + v * v
            ms = jnp.sum(total, axis=-1, keepdims=True) * (1.0 / 4096.0)
            scale = lax.rsqrt(ms + EPS)
            for fb in range(8):
                v = hb[fb, at, :].astype(F32)
                nb[at, fb * 512:(fb + 1) * 512] = (
                    v * scale * g_ref[:, fb * 512:(fb + 1) * 512]).astype(BF16)
            return 0

        lax.fori_loop(j * 16 + part * 4, j * 16 + part * 4 + 4, norm_rows, 0)

    def headmask():
        return lax.broadcasted_iota(jnp.int32, (LEN, 256), 1) // DH

    def soften(q, cc, j):
        head = headmask()
        who = c if cc == 0 else oc
        at = slice((j * 2 + q) * LEN, (j * 2 + q + 1) * LEN)
        qq, kk = qkv[0, who, at, :], qkv[1, who, at, :]
        zero = jnp.zeros((), BF16)
        qm = jnp.concatenate([jnp.where(head == h, qq, zero) for h in range(4)], axis=0)
        s = lax.dot_general(qm, kk, NT, preferred_element_type=F32) + bt[who]
        seen = mks[q, pl.ds(2 * c + j, 1), :]
        s = jnp.where(seen > 0.5, s, -1e30)
        top = jnp.max(s, axis=-1, keepdims=True)
        e = jnp.exp(s - top)
        wts[j, q, cc] = (e / jnp.sum(e, axis=-1, keepdims=True)).astype(BF16)

    def attend(q, cc, j):
        head = headmask()
        who = c if cc == 0 else oc
        at = slice((j * 2 + q) * LEN, (j * 2 + q + 1) * LEN)
        mix = jnp.dot(wts[j, q, cc], qkv[2, who, at, :], preferred_element_type=F32)
        out = jnp.zeros((LEN, 256), F32)
        for h in range(4):
            out = jnp.where(head == h, mix[h * LEN:(h + 1) * LEN], out)
        att[who, at, :] = out.astype(BF16)

    tasks, order, _, _ = list_schedule()
    landed = set()
    for t in order:
        for n in tasks[t][2]:
            if tasks[n][0] and n not in landed:
                land(n)
                landed.add(n)
        gate(t)
        issue(t)
    for t in order:
        if tasks[t][0] and t[0] != "fin" and t not in landed:
            land(t)
    for j in range(2):
        recv(o_ref.at[pl.ds((oc * 2 + j) * LEN, LEN)], fin.at[j])
    for d in outs:
        d.wait()
    for d in pending:
        d.wait_send()


def local(hidden_states, norm_gain, query_weight, keyvalue_weight, output_weight,
          position_bias, lengths):
    hbm = pl.BlockSpec(memory_space=pl.ANY)
    dma = pltpu.SemaphoreType.DMA
    return pl.pallas_call(
        kernel,
        out_shape=jax.ShapeDtypeStruct((512, 512), BF16),
        in_specs=[hbm] * 7,
        out_specs=hbm,
        scratch_shapes=[
            pltpu.VMEM((4, 2, 2, 4, 4, 128, 256), BF16),
            pltpu.VMEM((8, 512, 512), BF16),
            pltpu.VMEM((512, 4096), BF16),
            pltpu.VMEM((3, 2, 512, 256), BF16),
            pltpu.VMEM((2, 512, 256), BF16),
            pltpu.VMEM((8, 512, 512), F32),
            pltpu.VMEM((2, 4, 2, 2, 128, 512), BF16),
            pltpu.VMEM((2, 4, 2, 2, 128, 512), BF16),
            pltpu.VMEM((2, 512, 128), F32),
            pltpu.VMEM((2, BUCKETS, 8, LEN), F32),
            pltpu.VMEM((2, 8, LEN), F32),
            pltpu.VMEM((2, 128, 512), BF16),
            pltpu.VMEM((2, 128, 512), BF16),
            pltpu.VMEM((2, 2, 2, 512, 128), BF16),
            pltpu.VMEM((128, 512), BF16),
            pltpu.VMEM((128, 512), BF16),
            pltpu.VMEM((128, 2, 512), BF16),
            pltpu.VMEM((2, 128, 512), BF16),
            pltpu.VMEM((1, 4096), F32),
            pltpu.VMEM((8, BUCKETS), F32),
            pltpu.SMEM((4,), jnp.int32),
            dma((14,)),
            dma((1,)),
            dma((2, 4, 2, 2)),
            dma((2,)),
            dma((4,)),
            dma((2, 4, 2)),
            dma((2, 4)),
            dma((2, 4, 4, 2)),
            dma((2, 4, 4)),
            dma((2, 4, 7)),
            dma((2, 4, 2, 2)),
            dma((2,)),
            dma((2,)),
        ],
        compiler_params=pltpu.CompilerParams(
            collective_id=0, has_side_effects=True, vmem_limit_bytes=60 * 1024 * 1024),
        name="t5_attention",
    )(hidden_states, norm_gain, query_weight[0], keyvalue_weight[0], output_weight[0],
      jnp.transpose(position_bias[0]), lengths)


def solution(mesh):
    in_specs = (
        P("dp", "mp"),
        P(),
        P(None, "dp", "mp"),
        P(None, "dp", None, "mp"),
        P(None, "dp", "mp"),
        P(None, None, "mp"),
        P("dp"),
    )
    return jax.shard_map(local, mesh=mesh, in_specs=in_specs, out_specs=P("dp", "mp"), check_vma=False)
```

```python
import functools

import jax
import jax.numpy as jnp
import numpy as np
from jax import lax
from jax.experimental import pallas as pl
from jax.experimental.pallas import tpu as pltpu
from jax.sharding import PartitionSpec as P

MESH = pl.DeviceIdType.MESH
DH = 64
BUCKETS = 32
DIST = 128
LEN = 128
EPS = 1e-06
F32 = jnp.float32
BF16 = jnp.bfloat16
NT = (((1,), (1,)), ((), ()))


def far_steps():
    half = BUCKETS // 2
    exact = half // 2
    distance = np.arange(LEN)
    scaled = np.log(np.maximum(distance, 1) / exact) / np.log(DIST / exact) * (half - exact)
    far = np.minimum(exact + np.floor(scaled + 1e-09).astype(np.int32), half - 1)
    near = np.where(distance < exact, distance, far)
    return [int(np.min(distance[near >= b])) for b in range(1, half) if np.any(near >= b)]


STEPS = far_steps()


LINKS = ("x+", "x-", "y+", "y-", "zp", "zn", "d")
RATE = {"d": 500e3}
COST = {"norm": 0.45, "proj": 0.35, "soft": 0.28, "attn": 0.12, "out": 0.4, "bias": 0.5, "rs": 0.2, "fin": 0.3,
        "prep": 1.0, "small": 0.4}
AHEAD = 2.7
HOLD = 0.1


H_HOPS = {(0, 0): 3, (1, 0): 4, (0, 1): 3, (1, 1): 4}
R_HOPS = {(0, 0): 4, (1, 0): 3, (0, 1): 3, (1, 1): 4}


def flip(d):
    return {"+": "-", "-": "+", "p": "n", "n": "p"}[d]


def rounds(hops, d, r):
    side = d if r % 2 == 0 else flip(d)
    return hops if side == "p" else 7 - hops


OUT_NEED = {("p", 0): ("own",), ("p", 1): ("p",), ("p", 2): ("p",), ("p", 3): ("far",),
            ("n", 0): ("n",), ("n", 1): ("n",), ("n", 2): ("far",), ("n", 3): ("far",)}
RANK = {'zx': (-62.8, -38.1, 16.7, -3.3), 'h': (22.2, 71.8), 'w': (1.9, 27.0, 3.6, 30.5), 'f': -8.7, 's0': -46.4, 's1': 5.5, 's3': 28.7, 'f2': -21.6, 's2': -36.9, 'r': -21.5}


def make_tasks():
    tasks = {}

    def add(tid, link, kib, needs, rank):
        tasks[tid] = (link, kib, tuple(needs), rank)

    add(("prep",), None, 0, (), 0.2)
    add(("small",), None, 0, [("prep",)], 30)
    for j in range(2):
        add(("HD", j), "d", 128, (), 0)
    for m in range(4):
        add(("ZX", m), "zp", 64, [("prep",)] if m in (1, 2) else (), RANK["zx"][m])
    for j in range(2):
        for d in "pn":
            for r in range(4):
                for hh in range(2):
                    if r >= rounds(H_HOPS[hh, j], d, r):
                        continue
                    need = [("HD", j)] if r == 0 and hh == 1 else []
                    if r > 0:
                        need = [("H", flip(d), r - 1, hh, j)]
                    add(("H", d, r, hh, j), "z" + d, 128, need, RANK["h"][j] + r)
    for m in range(4):
        late = RANK["w"][m]
        for cls in range(2):
            fa, sa = ("x", "y") if cls == 0 else ("y", "x")
            base = [("ZX", m)] if cls else [("prep",)] if m in (1, 2) else []
            for d in "+-":
                add(("F", cls, m, d), fa + d, 64, base, late + RANK["f"])
                add(("S", cls, m, 0, d), sa + d, 64, base, late + RANK["s0"])
                add(("S", cls, m, 1, d), sa + d, 64, [("F", cls, m, "+")], late + RANK["s1"])
                add(("S", cls, m, 2, d), sa + d, 64, [("F", cls, m, "-")], late + RANK["s1"])
                add(("S", cls, m, 3, d), sa + d, 64, [("F2", cls, m)], late + RANK["s3"])
            d = "+-"[(m + cls) % 2]
            add(("F2", cls, m), fa + d, 64, [("F", cls, m, d)], late + RANK["f2"])
            for o in range(4):
                d = "+-"[(m + cls + o) % 2]
                add(("S2", cls, m, o), sa + d, 64, [("S", cls, m, o, d)], late + RANK["s2"])
                if o < 3:
                    add(("D", cls, m, o), "d", 256,
                        [("S", cls, m, o, "+"), ("S", cls, m, o, "-"), ("S2", cls, m, o)]
                        + ([("small",)] if o == 0 else []), late)
                    continue
                for i, need in enumerate((("F2", cls, m), ("S", cls, m, o, "+"), ("S", cls, m, o, "-"), ("S2", cls, m, o))):
                    add(("D", cls, m, o + i), "d", 64, [need], late)

    def mine(m):
        return ([("ZX", m)] + [("F", c, m, d) for c in range(2) for d in "+-"]
                + [("F2", c, m) for c in range(2)]
                + [("S", c, m, o, d) for c in range(2) for o in range(4) for d in "+-"]
                + [("S2", c, m, o) for c in range(2) for o in range(4)])

    def theirs(m):
        return [("D", c, m, o) for c in range(2) for o in range(7)]

    for i in range(4):
        add(("bias", i), None, 0, [("small",)], 60)
    for j in range(2):
        pieces = [("HD", j)] + [t for t in tasks if t[0] == "H" and t[4] == j]
        for i in range(4):
            add(("norm", j, i), None, 0, pieces, 40 + j)
        normed = [("norm", j, i) for i in range(4)] + [("small",)]
        for m in range(3):
            for cc in range(2):
                pieces = theirs(m) if cc else mine(m)
                for part in range(2):
                    need = [t for t in pieces if (1 if t[0] == "ZX" else t[1]) == part]
                    if part:
                        need.append(("proj", m, cc, j, 0))
                    add(("proj", m, cc, j, part), None, 0, normed + need, 42 + cc + 20 * j + 2 * m)
        for cc in range(2):
            for q in range(2):
                add(("soft", q, cc, j), None, 0,
                    [("bias", i) for i in range(4)] + [("proj", m, cc, j, 1) for m in range(2)], 48 + 20 * j)
                add(("attn", q, cc, j), None, 0, [("soft", q, cc, j), ("proj", 2, cc, j, 1)], 48 + 20 * j)
        for n, step in enumerate(("far", "n", "p", "own")):
            add(("out", step, j), None, 0,
                [("attn", q, cc, j) for q in range(2) for cc in range(2)] + mine(3) + theirs(3),
                50 + 20 * j + n)
        for d in "pn":
            for r in range(4):
                for hh in range(2):
                    hops = rounds(R_HOPS[hh, j], d, r)
                    if r >= hops:
                        continue
                    need = [("out", step, j) for step in (OUT_NEED[d, r])]
                    if r < hops - 1:
                        need.append(("R", flip(d), r + 1, hh, j))
                    add(("R", d, r, hh, j), "z" + d, 128, need, 33 + RANK["r"] * j - r)
        for hh in (1, 0):
            add(("fin", hh, j), "d" if hh else None, 128,
                [("out", "own", j), ("R", "p", 0, hh, j), ("R", "n", 0, hh, j)], 30 + j)
    return tasks


def list_schedule():
    tasks = make_tasks()
    free = dict.fromkeys(LINKS, 0.0)
    arrive, finished, order = {}, {}, []
    left = dict(tasks)
    now, summing = 0.0, False

    def ready_at(tid):
        t = 0.0
        for n in tasks[tid][2]:
            when = arrive.get(n) if tasks[n][0] else finished.get(n)
            if when is None:
                return None
            t = max(t, when)
        return t

    while left:
        best, soonest, due = None, None, None
        for tid in left:
            link, kib, _, rank = tasks[tid]
            at = ready_at(tid)
            if at is None:
                continue
            links = (link,) if link else ()
            for one in links:
                at = max(at, free[one] - AHEAD)
            if at <= now + 1e-9:
                key = (0 if link else 1, rank, str(tid))
                if best is None or key < best[0]:
                    best = (key, tid, links)
            else:
                soonest = at if soonest is None else min(at, soonest)
                if link:
                    due = at if due is None else min(at, due)
        if best is None:
            now = soonest
            continue
        _, tid, links = best
        if summing and not links and due is not None and due < now + COST.get(tid[0], 0.06) - HOLD:
            now = due
            continue
        summing = summing or tid[0] == "R"
        link, kib, _, _ = tasks[tid]
        kind = {"R": "rs"}.get(tid[0], tid[0])
        now += COST.get(kind, 0.06)
        finished[tid] = now
        if link:
            rate = RATE.get(link, 46.0e3) / 1.024e3
            t = max([now] + [free[one] for one in links]) + kib / rate
            for one in links:
                free[one] = t
            arrive[tid] = t + (1.0 if link == "d" else 1.8)
        order.append(tid)
        del left[tid]
    return tasks, order, finished, arrive


def kernel(x_ref, g_hbm, q_hbm, kv_hbm, ow_hbm, pb_hbm, len_hbm, o_ref,
           wb, hb, nb, qkv, att, ob, sb, rb, bt, pbs, mks, fs, fr, wts, acc,
           wq, wo, wkv, kvs, g_ref, pbv, lens,
           loc_sem, send_sem, hr, hd, wzs, wf, wf2, ws, ws2, wd, rr, sm, fin):
    dp = lax.axis_index("dp")
    mp = lax.axis_index("mp")
    zl, xi, yi = dp // 16, (dp // 4) % 4, dp % 4
    zh, c = mp // 2, mp % 2
    z = zh * 2 + zl
    oc = 1 - c
    oz = 1 - zl

    toward = 1 - 2 * zl

    def zstep(d, n):
        return (z + 8 + (toward if d == "p" else -toward) * n) % 8

    def dev(zz, xx, yy, cc):
        return ((zz % 2) * 16 + xx * 4 + yy, (zz // 2) * 2 + cc)

    xp, xm = (xi + 1) % 4, (xi + 3) % 4
    yp, ym = (yi + 1) % 4, (yi + 3) % 4
    devices = {
        "x+": dev(z, xp, yi, c), "x-": dev(z, xm, yi, c),
        "y+": dev(z, xi, yp, c), "y-": dev(z, xi, ym, c),
        "zp": dev(zstep("p", 1), xi, yi, c), "zn": dev(zstep("n", 1), xi, yi, c),
        "d": dev(z, xi, yi, oc),
    }
    pending, outs = [], []

    def send(src, dst, sem, link):
        d = pltpu.make_async_remote_copy(
            src_ref=src, dst_ref=dst, send_sem=send_sem.at[0], recv_sem=sem,
            device_id=devices[link], device_id_type=MESH)
        d.start()
        pending.append(d)

    def recv(dst, sem):
        pltpu.make_async_remote_copy(
            src_ref=dst, dst_ref=dst, send_sem=send_sem.at[0], recv_sem=sem,
            device_id=devices["d"], device_id_type=MESH).wait_recv()

    lanes = pl.ds(pl.multiple_of(zl * 256, 256), 256)
    far_lanes = pl.ds(pl.multiple_of(oz * 256, 256), 256)

    def source(m, at):
        if m == 0:
            return wq.at[:, at]
        if m == 3:
            return wo.at[:, at]
        return kvs.at[m - 1, :, at]

    def col(zz, hh):
        return (zz // 2) * 2 + (c if hh == 0 else oc)

    def rows(zz, j):
        return pl.ds(pl.multiple_of((j * 2 + zz % 2) * LEN, LEN), LEN)

    def local(i, src, dst):
        d = pltpu.make_async_copy(src, dst, loc_sem.at[i])
        d.start()
        return d

    own_x = [local(j, x_ref.at[pl.ds((c * 2 + j) * LEN, LEN)], hb.at[mp, rows(z, j)]) for j in range(2)]
    own_q = local(2, q_hbm, wq)
    own_kv = local(3, kv_hbm, wkv)
    own_o = local(4, ow_hbm, wo)
    rest = [local(5, pb_hbm, pbv), local(6, len_hbm, lens), local(7, g_hbm, g_ref),
            local(8, q_hbm.at[:, lanes], wb.at[0, c, zl, xi, yi]),
            local(9, ow_hbm.at[:, lanes], wb.at[3, c, zl, xi, yi])]

    barrier = pltpu.get_barrier_semaphore()
    for link in LINKS:
        pl.semaphore_signal(barrier, inc=1, device_id=devices[link], device_id_type=MESH)
    pl.semaphore_wait(barrier, len(LINKS))

    def blk(m, cls, f, s):
        bx, by = (f, s) if cls == 0 else (s, f)
        return wb.at[m, c, zl if cls == 0 else oz, bx, by]

    def axes(cls):
        return ("x", "y", xi, yi) if cls == 0 else ("y", "x", yi, xi)

    def step(i, d):
        return (i + (1 if d == "+" else 3)) % 4

    def fblock(cls, o):
        f = axes(cls)[2]
        return (f + (0, 3, 1, 2)[o]) % 4

    def dslice(m, cls, o, cc):
        f, s = axes(cls)[2:]
        ff = fblock(cls, min(o, 3))
        if o >= 3:
            s = (s + (0, 3, 1, 2)[o - 3]) % 4
            bx, by = (ff, s) if cls == 0 else (s, ff)
            return wb.at[m, cc, zl if cls == 0 else oz, bx, by]
        if cls == 0:
            return wb.at[m, cc, zl, ff]
        return wb.at[m, cc, oz, :, ff]

    def hpiece(zo, hh, j):
        return hb.at[col(zo, hh), rows(zo, j)]

    def side(d):
        return 0 if d in "+p" else 1

    waits = {"x0": own_x[0], "x1": own_x[1], "q": own_q, "o": own_o}

    def gate(t):
        key = None
        if t[0] == "H" and t[2] == 0 and t[3] == 0:
            key = "x%d" % t[4]
        elif t[0] in ("ZX", "F", "S"):
            m = t[1] if t[0] == "ZX" else t[2]
            key = {0: "q", 3: "o"}.get(m)
        if key in waits:
            waits.pop(key).wait()

    def issue(t):
        kind = t[0]
        if kind == "HD":
            send(x_ref.at[pl.ds((oc * 2 + t[1]) * LEN, LEN)], hb.at[mp, rows(z, t[1])], hd.at[t[1]], "d")
        elif kind == "ZX":
            send(source(t[1], far_lanes), wb.at[t[1], c, zl, xi, yi], wzs.at[t[1]], "zp")
        elif kind == "H":
            _, d, r, hh, j = t
            p = hpiece(zstep(flip(d), r), hh, j)
            send(p, p, hr.at[side(d), r, hh, j], "z" + d)
        elif kind == "F":
            _, cls, m, d = t
            fa, sa, f, s = axes(cls)
            own = blk(m, cls, f, s)
            send(source(m, lanes) if cls == 0 else own, own, wf.at[cls, m, side(d)], fa + d)
        elif kind == "F2":
            _, cls, m = t
            fa, sa, f, s = axes(cls)
            d = "+-"[(m + cls) % 2]
            b = blk(m, cls, step(f, flip(d)), s)
            send(b, b, wf2.at[cls, m], fa + d)
        elif kind == "S":
            _, cls, m, o, d = t
            fa, sa, f, s = axes(cls)
            b = blk(m, cls, fblock(cls, o), s)
            send(source(m, lanes) if cls == 0 and o == 0 else b, b, ws.at[cls, m, o, side(d)], sa + d)
        elif kind == "S2":
            _, cls, m, o = t
            fa, sa, f, s = axes(cls)
            d = "+-"[(m + cls + o) % 2]
            b = blk(m, cls, fblock(cls, o), step(s, flip(d)))
            send(b, b, ws2.at[cls, m, o], sa + d)
        elif kind == "D":
            _, cls, m, o = t
            p = dslice(m, cls, o, c)
            send(p, p, wd.at[cls, m, o], "d")
        elif kind == "R":
            _, d, r, hh, j = t
            dz = zstep(d, r + 1)
            value = ob[col(dz, hh), rows(dz, j), :]
            if r < rounds(R_HOPS[hh, j], d, r) - 1:
                value = value + rb[side(flip(d)), r + 1, hh, j].astype(F32)
            sb[side(d), r, hh, j] = value.astype(BF16)
            send(sb.at[side(d), r, hh, j], rb.at[side(d), r, hh, j], rr.at[side(d), r, hh, j], "z" + d)
        elif kind == "fin":
            _, hh, j = t
            value = (hb[col(z, hh), rows(z, j), :].astype(F32) + ob[col(z, hh), rows(z, j), :]
                     + rb[0, 0, hh, j].astype(F32) + rb[1, 0, hh, j].astype(F32)).astype(BF16)
            if hh:
                fs[j] = value
                send(fs.at[j], o_ref.at[pl.ds((c * 2 + j) * LEN, LEN)], fin.at[j], "d")
            else:
                fr[j] = value
                outs.append(local(12 + j, fr.at[j], o_ref.at[pl.ds((c * 2 + j) * LEN, LEN)]))
        elif kind == "prep":
            prep()
        elif kind == "small":
            small()
        elif kind == "bias":
            bias(t[1])
        elif kind == "norm":
            norm(t[1], t[2])
        elif kind == "proj":
            _, m, cc, j, part = t
            who = c if cc == 0 else oc
            zz = oz if part else zl
            half = slice(j * 256, j * 256 + 256)
            depth = pl.ds(pl.multiple_of(zz * 2048, 2048), 2048)
            value = jnp.dot(nb[half, depth], wb[m, who, zz].reshape(2048, 256), preferred_element_type=F32)
            if part:
                qkv[m, who, half, :] = (value + acc[m, cc, j]).astype(BF16)
            else:
                acc[m, cc, j] = value
        elif kind == "soft":
            soften(*t[1:])
        elif kind == "attn":
            attend(*t[1:])
        elif kind == "out":
            zq = {"own": zh, "p": zstep("p", 2) // 2, "n": zstep("n", 1) // 2, "far": (zh + 2) % 4}[t[1]]
            half = slice(t[2] * 256, t[2] * 256 + 256)
            for hh in range(2):
                fb = zq * 2 + hh
                total = None
                for cc in range(2):
                    w = wb[3, cc, fb // 4, fb % 4].reshape(512, 256)
                    part = lax.dot_general(att[cc, half, :], w, NT, preferred_element_type=F32)
                    total = part if total is None else total + part
                ob[fb, half, :] = total

    def land(t):
        kind = t[0]
        if kind == "HD":
            recv(hb.at[zh * 2 + oc, rows(z, t[1])], hd.at[t[1]])
        elif kind == "ZX":
            recv(blk(t[1], 1, yi, xi), wzs.at[t[1]])
        elif kind == "H":
            _, d, r, hh, j = t
            recv(hpiece(zstep(d, r + 1), hh, j), hr.at[side(d), r, hh, j])
        elif kind == "F":
            _, cls, m, d = t
            fa, sa, f, s = axes(cls)
            recv(blk(m, cls, step(f, flip(d)), s), wf.at[cls, m, side(d)])
        elif kind == "F2":
            _, cls, m = t
            fa, sa, f, s = axes(cls)
            recv(blk(m, cls, (f + 2) % 4, s), wf2.at[cls, m])
        elif kind == "S":
            _, cls, m, o, d = t
            fa, sa, f, s = axes(cls)
            recv(blk(m, cls, fblock(cls, o), step(s, flip(d))), ws.at[cls, m, o, side(d)])
        elif kind == "S2":
            _, cls, m, o = t
            fa, sa, f, s = axes(cls)
            recv(blk(m, cls, fblock(cls, o), (s + 2) % 4), ws2.at[cls, m, o])
        elif kind == "D":
            _, cls, m, o = t
            recv(dslice(m, cls, o, oc), wd.at[cls, m, o])
        elif kind == "R":
            _, d, r, hh, j = t
            recv(rb.at[side(d), r, hh, j], rr.at[side(d), r, hh, j])

    def prep():
        own_kv.wait()
        for i in range(2):
            kvs[i] = wkv[:, i, :]
            rest.append(local(10 + i, kvs.at[i, :, lanes], wb.at[1 + i, c, zl, xi, yi]))

    def small():
        for d in rest:
            d.wait()
        for b in range(BUCKETS):
            pbs[c, b] = jnp.broadcast_to(pbv[:, b:b + 1], (8, LEN))
        lane = lax.broadcasted_iota(jnp.int32, (1, LEN), 1)
        for i in range(4):
            mks[zl, pl.ds(i, 1), :] = jnp.where(lane < lens[i], 1.0, 0.0)
        send(pbs.at[c], pbs.at[c], sm.at[0], "d")
        send(mks.at[zl], mks.at[zl], sm.at[1], "zp")

    def bias(part):
        if part == 0:
            recv(mks.at[oz], sm.at[1])
        if part == 2:
            recv(pbs.at[oc], sm.at[0])
        row = lax.broadcasted_iota(jnp.int32, (LEN, LEN), 0)
        lane = lax.broadcasted_iota(jnp.int32, (LEN, LEN), 1)
        rel = lane - row
        dist = jnp.abs(rel)
        bucket = jnp.where(rel > 0, BUCKETS // 2, 0)
        for t in STEPS:
            bucket = bucket + jnp.where(dist >= t, 1, 0)

        def bias_head(i, _):
            cc, h = c if part < 2 else oc, i % 4
            tab = jnp.zeros((LEN, LEN), F32)
            for b in range(BUCKETS):
                tab = jnp.where(bucket == b, pbs[cc, b, pl.ds(zl * 4 + h, 1), :], tab)
            bt[cc, pl.ds(pl.multiple_of(h * LEN, LEN), LEN), :] = tab
            return 0

        lax.fori_loop(part * 2, part * 2 + 2, bias_head, 0)

    def norm(j, part):
        def norm_rows(i, _):
            at = pl.ds(pl.multiple_of(i * 16, 16), 16)
            total = jnp.zeros((16, 512), F32)
            for fb in range(8):
                v = hb[fb, at, :].astype(F32)
                total = total + v * v
            ms = jnp.sum(total, axis=-1, keepdims=True) * (1.0 / 4096.0)
            scale = lax.rsqrt(ms + EPS)
            for fb in range(8):
                v = hb[fb, at, :].astype(F32)
                nb[at, fb * 512:(fb + 1) * 512] = (
                    v * scale * g_ref[:, fb * 512:(fb + 1) * 512]).astype(BF16)
            return 0

        lax.fori_loop(j * 16 + part * 4, j * 16 + part * 4 + 4, norm_rows, 0)

    def headmask():
        return lax.broadcasted_iota(jnp.int32, (LEN, 256), 1) // DH

    def soften(q, cc, j):
        head = headmask()
        who = c if cc == 0 else oc
        at = slice((j * 2 + q) * LEN, (j * 2 + q + 1) * LEN)
        qq, kk = qkv[0, who, at, :], qkv[1, who, at, :]
        zero = jnp.zeros((), BF16)
        qm = jnp.concatenate([jnp.where(head == h, qq, zero) for h in range(4)], axis=0)
        s = lax.dot_general(qm, kk, NT, preferred_element_type=F32) + bt[who]
        seen = mks[q, pl.ds(2 * c + j, 1), :]
        s = jnp.where(seen > 0.5, s, -1e30)
        top = jnp.max(s, axis=-1, keepdims=True)
        e = jnp.exp(s - top)
        wts[j, q, cc] = (e / jnp.sum(e, axis=-1, keepdims=True)).astype(BF16)

    def attend(q, cc, j):
        head = headmask()
        who = c if cc == 0 else oc
        at = slice((j * 2 + q) * LEN, (j * 2 + q + 1) * LEN)
        mix = jnp.dot(wts[j, q, cc], qkv[2, who, at, :], preferred_element_type=F32)
        out = jnp.zeros((LEN, 256), F32)
        for h in range(4):
            out = jnp.where(head == h, mix[h * LEN:(h + 1) * LEN], out)
        att[who, at, :] = out.astype(BF16)

    tasks, order, _, _ = list_schedule()
    landed = set()
    for t in order:
        for n in tasks[t][2]:
            if tasks[n][0] and n not in landed:
                land(n)
                landed.add(n)
        gate(t)
        issue(t)
    for t in order:
        if tasks[t][0] and t[0] != "fin" and t not in landed:
            land(t)
    for j in range(2):
        recv(o_ref.at[pl.ds((oc * 2 + j) * LEN, LEN)], fin.at[j])
    for d in outs:
        d.wait()
    for d in pending:
        d.wait_send()


def local(hidden_states, norm_gain, query_weight, keyvalue_weight, output_weight,
          position_bias, lengths):
    hbm = pl.BlockSpec(memory_space=pl.ANY)
    dma = pltpu.SemaphoreType.DMA
    return pl.pallas_call(
        kernel,
        out_shape=jax.ShapeDtypeStruct((512, 512), BF16),
        in_specs=[hbm] * 7,
        out_specs=hbm,
        scratch_shapes=[
            pltpu.VMEM((4, 2, 2, 4, 4, 128, 256), BF16),
            pltpu.VMEM((8, 512, 512), BF16),
            pltpu.VMEM((512, 4096), BF16),
            pltpu.VMEM((3, 2, 512, 256), BF16),
            pltpu.VMEM((2, 512, 256), BF16),
            pltpu.VMEM((8, 512, 512), F32),
            pltpu.VMEM((2, 4, 2, 2, 128, 512), BF16),
            pltpu.VMEM((2, 4, 2, 2, 128, 512), BF16),
            pltpu.VMEM((2, 512, 128), F32),
            pltpu.VMEM((2, BUCKETS, 8, LEN), F32),
            pltpu.VMEM((2, 8, LEN), F32),
            pltpu.VMEM((2, 128, 512), BF16),
            pltpu.VMEM((2, 128, 512), BF16),
            pltpu.VMEM((2, 2, 2, 512, 128), BF16),
            pltpu.VMEM((3, 2, 2, 256, 256), F32),
            pltpu.VMEM((128, 512), BF16),
            pltpu.VMEM((128, 512), BF16),
            pltpu.VMEM((128, 2, 512), BF16),
            pltpu.VMEM((2, 128, 512), BF16),
            pltpu.VMEM((1, 4096), F32),
            pltpu.VMEM((8, BUCKETS), F32),
            pltpu.SMEM((4,), jnp.int32),
            dma((14,)),
            dma((1,)),
            dma((2, 4, 2, 2)),
            dma((2,)),
            dma((4,)),
            dma((2, 4, 2)),
            dma((2, 4)),
            dma((2, 4, 4, 2)),
            dma((2, 4, 4)),
            dma((2, 4, 7)),
            dma((2, 4, 2, 2)),
            dma((2,)),
            dma((2,)),
        ],
        compiler_params=pltpu.CompilerParams(
            collective_id=0, has_side_effects=True, vmem_limit_bytes=60 * 1024 * 1024),
        name="t5_attention",
    )(hidden_states, norm_gain, query_weight[0], keyvalue_weight[0], output_weight[0],
      jnp.transpose(position_bias[0]), lengths)


def solution(mesh):
    in_specs = (
        P("dp", "mp"),
        P(),
        P(None, "dp", "mp"),
        P(None, "dp", None, "mp"),
        P(None, "dp", "mp"),
        P(None, None, "mp"),
        P("dp"),
    )
    return jax.shard_map(local, mesh=mesh, in_specs=in_specs, out_specs=P("dp", "mp"), check_vma=False)
```
